256 devices in a mesh: rows: 64 (over z, x, core), grp: 4 (over y).
Axes of the slice: x: 4, y: 4, z: 8, core: 2. Of those that a mesh axis runs over, the one named last changes fastest.
Arguments:
- user_features: bfloat16 [4, 16384, 256], P('grp', 'rows'), may hold values from -72 to 72
- w_first: bfloat16 [256, 256], replicated, may hold values from -0.375 to 0.375
- w_second: bfloat16 [256, 256], replicated, may hold values from -0.375 to 0.375
- item_embed: bfloat16 [4, 16384, 256], P('grp', 'rows'), may hold values from -27 to 27
- example_weight: float32 [4, 16384], P('grp', 'rows'), may hold values from 0.02 to 0.2
- positive: int32 [4, 16384], P('grp', 'rows'), may hold values from 0 to 16383
- item_owner: int32 [4, 16384, 1], P('grp', 'rows'), may hold values from 0 to 63; in each aligned block of 256 rows (0 to 255, 256 to 511, ..., all dimensions but the last counted through in order) at most 16 rows name the same one
- item_row: int32 [4, 16384], P('grp', 'rows'), may hold values from 0 to 4095
Outputs:
- grad_first: float32 [256, 256], replicated
- grad_second: float32 [256, 256], replicated
- grad_table: float32 [262144, 256], P('rows', 'grp')
The draws below stay inside these ranges and needn't reach their ends.
Inputs may be any that keep to these rules, and one draw needn't show every extreme that they name: `item_owner`: within the rows of one device (aligned blocks of 256 pairs of a group) no owner is named by more than 16 pairs, a bound that some block reaches.
All inputs are finite; a program needn't handle non-finite values.
Results may differ from the reference program's by a relative error of at most 0.0023.
The reference program's roundings to bfloat16 on the way count: a program that leaves them out, or rounds other values in their place, can miss the bound.
Values may be sent and summed in bfloat16 or wider, within the bound.
A program may use at most 128 MiB of HBM per device.

```python
import math
import jax
import jax.numpy as jnp
import numpy as np
from jax import lax

D = 256
DIN = 256
DH = 256
BATCH_DEV = 256
ITEMS_DEV = 4096
GU = 16384
CAP = 16
N_ROWS = 64
N_GRP = 4


def draw_user_features(key, part):
    first_key = jax.random.fold_in(jax.random.fold_in(key, 11), 0)
    values = jnp.clip(jax.random.normal(first_key, (N_GRP, GU, DIN), jnp.float32), -6.0, 6.0)
    return values.astype(jnp.bfloat16)


def draw_item_embed(key, part):
    first_key = jax.random.fold_in(jax.random.fold_in(key, 23), 0)
    values = 0.15 * jnp.clip(jax.random.normal(first_key, (N_GRP, GU, D), jnp.float32), -6.0, 6.0)
    return values.astype(jnp.bfloat16)


def with_ends(entries, own_key, least, top_value):
    dims = entries.shape
    place = [jax.random.randint(jax.random.fold_in(own_key, axis), (), 0, dims[axis]) for axis in range(len(dims))]
    entries = entries.at[tuple(place)].set(least)
    longest = dims.index(max(dims))
    place[longest] = (place[longest] + 1) % dims[longest]
    return entries.at[tuple(place)].set(top_value)


def shard_levels(rng, dims, shards, low, largest):
    gain = 1.0
    for axis_at, shards_of in shards:
        draws = jax.random.uniform(jax.random.fold_in(jax.random.fold_in(rng, 6), axis_at), (shards_of,), jnp.float32, low / len(shards), largest / len(shards))
        gain = gain * jnp.repeat(jnp.exp(draws), dims[axis_at] // shards_of).reshape((-1,) + (1,) * (len(dims) - 1 - axis_at))
    return gain


def cumulative_ranks(number_of, slope):
    loads = [(1 << 20) // math.isqrt(standing ** slope) + 1 for standing in range(1, number_of + 1)]
    width = 1 + sum(loads) // (1 << 30)
    return np.cumsum(np.array([max(1, weight // width) for weight in loads]))


def ranked_ids(own_key, extent, amount, lean):
    listing = cumulative_ranks(amount, lean)
    pick = jax.random.randint(jax.random.fold_in(own_key, 1), extent, 0, int(listing[amount - 1]))
    standing = jnp.searchsorted(jnp.asarray(listing, jnp.int32), pick, side="right")
    return jax.random.permutation(jax.random.fold_in(own_key, 2), amount)[standing].astype(jnp.int32)


def assign_block(rng, own, number, rows, count, top, limit, skew):
    ranking = jax.random.permutation(rng, count)
    packed, common = shares(count, rows * top, limit, skew, True), shares(count, rows * top, limit, skew, False)
    places = jnp.arange(count)

    def named(tallies, rotation):
        used = int((tallies > 0).sum())
        fixed = max(1, used // 4)
        passed = fixed + (places - fixed + rotation * (used - fixed)) % max(1, count - fixed)
        return jnp.zeros((count,), jnp.int32).at[ranking[jnp.where(places < fixed, places, passed)]].set(jnp.asarray(tallies, jnp.int32))

    tallies = jnp.where(number % 4 == 0, named(packed, number // 4), named(common, number - number // 4 - 1))
    mixed = jax.random.permutation(jax.random.fold_in(own, 3), count)
    donor, sink = mixed[0:count // 2 * 2:2], mixed[1:count // 2 * 2:2]
    room = jnp.minimum(tallies[donor] - 1, limit - tallies[sink]) // 2
    room = jnp.where((donor == ranking[0]) | (sink == ranking[0]) | (tallies[sink] == 0), 0, jnp.maximum(room, 0))
    passed = jax.random.randint(jax.random.fold_in(own, 4), (count // 2,), 0, 1 << 20) % (room + 1)
    tallies = tallies.at[donor].add(-passed).at[sink].add(passed)
    labels = jnp.searchsorted(jnp.cumsum(tallies), jnp.arange(rows * top), side="right").astype(jnp.int32)
    grid = labels.reshape(top, rows).T
    grid = grid[jax.random.permutation(jax.random.fold_in(own, 1), rows)]
    rotation = jax.random.randint(jax.random.fold_in(own, 2), (rows, 1), 0, top)
    return jnp.take_along_axis(grid, (jnp.arange(top)[None, :] + rotation) % top, axis=1)


def shares(amount, total, reach, skew, full):
    portions = [(1 << 20) // math.isqrt(grade ** skew) + 1 for grade in range(1, amount + 1)]
    largest = reach if full else min(reach, max(-(-total // amount), total * portions[0] // sum(portions)))
    least = 1 if total - largest >= amount - 1 else 0
    counts, surplus = [largest] + [least] * (amount - 1), total - largest - least * (amount - 1)
    while surplus > 0:
        candidates = [i for i in range(1, amount) if counts[i] < largest] or [i for i in range(1, amount) if counts[i] < reach]
        pool, remaining = sum([portions[i] for i in candidates]), surplus
        for i in candidates:
            more = min(reach - counts[i], max(1, remaining * portions[i] // pool), surplus)
            counts[i] = counts[i] + more
            surplus = surplus - more
    return np.array(counts)


def centred(rng, dims, scale, reach, held_as=jnp.bfloat16):
    array = scale * jax.random.normal(rng, dims, jnp.float32)
    return jnp.clip(array, min=-reach, max=reach).astype(held_as)


def setup_inputs(seed: int = 0) -> dict:
    key_list = jax.random.split(jax.random.key(seed), 9)
    user_features = draw_user_features(jax.random.fold_in(key_list[8], 71), 0)
    w_first = centred(key_list[1], (DIN, DH), DIN ** -0.5, 0.375)
    w_second = centred(key_list[2], (DH, D), DH ** -0.5, 0.375)
    item_embed = draw_item_embed(jax.random.fold_in(key_list[8], 71), 0)
    example_weight = jnp.clip(jnp.exp(math.log(0.2) - 2.3025851 * jax.random.uniform(key_list[4], (N_GRP, GU), jnp.float32) ** shard_levels(key_list[4], (N_GRP, GU), ((0, 4), (1, 64)), -0.2, 0.2)), 0.02, 0.2)
    positive = with_ends(jax.random.randint(key_list[5], (N_GRP, GU), 0, GU), jax.random.fold_in(key_list[5], 1), 0, GU - 1).astype(jnp.int32)
    item_owner_keys = jax.random.split(jax.random.fold_in(key_list[6], 1), N_GRP * GU // BATCH_DEV)
    item_owner_turns = jax.random.permutation(jax.random.fold_in(key_list[6], 3), N_GRP * GU // BATCH_DEV)
    item_owner = jax.vmap(lambda own, number: assign_block(jax.random.fold_in(key_list[6], 2), own, number, BATCH_DEV, N_ROWS, 1, CAP, 2))(item_owner_keys, item_owner_turns).reshape((N_GRP, GU, 1))
    item_row = with_ends(ranked_ids(key_list[7], (N_GRP, GU), ITEMS_DEV, 2), jax.random.fold_in(key_list[7], 3), 0, ITEMS_DEV - 1).astype(jnp.int32)
    return dict(user_features=user_features, w_first=w_first, w_second=w_second, item_embed=item_embed, example_weight=example_weight, positive=positive, item_owner=item_owner, item_row=item_row)


def reference(user_features, w_first, w_second, item_embed, example_weight, positive, item_owner, item_row):
    group_users = user_features.shape[1]
    row_block = math.gcd(group_users, 1024)
    num_blocks = group_users // row_block

    def one_group(inputs):
        features, group_items, weights, targets = inputs
        pre_act = jnp.dot(features, w_first, preferred_element_type=jnp.float32)
        hidden = jax.nn.silu(pre_act).astype(jnp.bfloat16)
        user_vecs = jnp.dot(hidden, w_second, preferred_element_type=jnp.float32).astype(jnp.bfloat16)
        items_wide = group_items.astype(jnp.float32)
        users_wide = user_vecs.astype(jnp.float32)
        columns = jnp.arange(group_users, dtype=jnp.int32)

        def block_step(accum, block_no):
            first_row = (block_no * row_block).astype(jnp.int32)
            user_block = lax.dynamic_slice_in_dim(users_wide, first_row, row_block, 0)
            weight_block = lax.dynamic_slice_in_dim(weights, first_row, row_block, 0)
            target_block = lax.dynamic_slice_in_dim(targets, first_row, row_block, 0)
            scores = jnp.dot(user_block, items_wide.T)
            row_max = jnp.max(scores, axis=1, keepdims=True)
            log_total = row_max + jnp.log(jnp.sum(jnp.exp(scores - row_max), axis=1, keepdims=True))
            chosen = (columns[None, :] == target_block[:, None]).astype(jnp.float32)
            dscore = (weight_block[:, None] * (jnp.exp(scores - log_total) - chosen)).astype(jnp.bfloat16)
            dscore_wide = dscore.astype(jnp.float32)
            grad_block = jnp.dot(dscore_wide, items_wide)
            accum = accum + jnp.dot(dscore_wide.T, user_block)
            return accum, grad_block

        grad_item, grad_blocks = lax.scan(block_step, jnp.zeros((group_users, D), jnp.float32),
                                          jnp.arange(num_blocks, dtype=jnp.int32))
        grad_user = grad_blocks.reshape(group_users, D).astype(jnp.bfloat16)
        d_second = jnp.dot(hidden.T, grad_user, preferred_element_type=jnp.float32)
        back_grad = jnp.dot(grad_user, w_second.T, preferred_element_type=jnp.float32)
        sigmoid_pre = jax.nn.sigmoid(pre_act)
        grad_pre = (back_grad * sigmoid_pre * (1.0 + pre_act * (1.0 - sigmoid_pre))).astype(jnp.bfloat16)
        d_first = jnp.dot(features.T, grad_pre, preferred_element_type=jnp.float32)
        return grad_item, d_first, d_second

    grad_item, d_first, d_second = lax.map(one_group, (user_features, item_embed, example_weight, positive))
    grad_first = jnp.sum(d_first, axis=0)
    grad_second = jnp.sum(d_second, axis=0)
    table_ids = (item_owner[:, :, 0] * ITEMS_DEV + item_row).astype(jnp.int32)
    grad_table = jax.ops.segment_sum(grad_item.reshape(-1, D), table_ids.reshape(-1),
                                     num_segments=ITEMS_DEV * N_ROWS)
    return grad_first, grad_second, grad_table
```

```python
import functools
import jax
import jax.numpy as jnp
from jax import lax
from jax.experimental import pallas as pl
from jax.experimental.pallas import tpu as pltpu
from jax.sharding import Mesh
from jax.sharding import PartitionSpec as P

ITEMS_DEV = 4096
ROWS = ("rows_0", "rows_1", "rows_2")
ROWS_GRP = ("rows_0", "rows_1", "rows_2", "grp")
MESH = pl.DeviceIdType.MESH
F32 = jnp.float32
BF16 = jnp.bfloat16


def chain_length(n, way, half):
    return n // 2 if (way == 0) == (half == 0) else n // 2 - 1


def contract(left, right, dims):
    return lax.dot_general(left, right, ((dims[:1], dims[1:]), ((), ())), preferred_element_type=F32)


def block_kernel(
    nz, nx, nc, feat_ref, w1_ref, w2_ref, items_ref, meta_ref, gi_ref, df_ref,
    users, items_all, items_turned, meta_all, peaks, sums, lses, scale, probs, ds,
    gi_part, gu_part, gu_pair, z_land, x_land, pre_keep, hid_keep,
    z_send, z_recv, x_send, x_recv, p_send, p_recv, m_send, m_recv, l_send, l_recv,
    zr_send, zr_recv, d_send, d_recv, xr_send, xr_recv,
):
    z, x, c = lax.axis_index("rows_0"), lax.axis_index("rows_1"), lax.axis_index("rows_2")
    size = items_ref.shape[0]
    half_size = size // 2
    peers = nx * nc
    me = x * nc + c
    signs = (1, -1)

    def z_at(step):
        return lax.rem(z + step + nz, nz)

    def x_at(step):
        return lax.rem(x + step + nx, nx)

    def peer(step):
        dx, dc = divmod(step, nc)
        return {"rows_1": x_at(dx), "rows_2": lax.rem(c + dc, nc)}

    def from_peer(step):
        dx, dc = divmod(step, nc)
        return x_at(-dx) * nc + lax.rem(c + nc - dc, nc)

    partner = {"rows_2": 1 - c}
    pending = []

    def send(src, dst, send_sem, recv_sem, where):
        copy = pltpu.make_async_remote_copy(
            src_ref=src, dst_ref=dst, send_sem=send_sem, recv_sem=recv_sem,
            device_id=where, device_id_type=MESH,
        )
        copy.start()
        pending.append(copy)

    def arrived(ref, recv_sem):
        pltpu.make_async_copy(ref, ref, recv_sem).wait()

    barrier = pltpu.get_barrier_semaphore()
    for step in range(1, peers):
        pl.semaphore_signal(barrier, inc=1, device_id=peer(step), device_id_type=MESH)
    for sign in signs:
        pl.semaphore_signal(
            barrier, inc=1, device_id={"rows_0": z_at(sign)}, device_id_type=MESH
        )

    def rows_of(block, half):
        return pl.ds(pl.multiple_of(block * size + half * half_size, half_size), half_size)

    def block_rows(block):
        return pl.ds(pl.multiple_of(block * size, size), size)

    pre = jnp.dot(feat_ref[...], w1_ref[...], preferred_element_type=F32)
    hidden = (pre * jax.nn.sigmoid(pre)).astype(BF16)
    hid_keep[...] = hidden
    users[block_rows(me), :] = jnp.dot(hidden, w2_ref[...], preferred_element_type=F32).astype(BF16)
    items_all[z] = items_ref[...]
    meta_all[me] = meta_ref[...]

    pl.semaphore_wait(barrier, peers - 1 + 2)

    def z_forward(r):
        for way, sign in enumerate(signs):
            for half in (0, 1):
                length = chain_length(nz, way, half)
                rows = pl.ds(half * half_size, half_size)
                if 1 <= r <= length:
                    arrived(items_all.at[z_at(-sign * r), rows], z_recv.at[way, half, r - 1])
                if r < length:
                    block = z_at(-sign * r)
                    src = items_ref.at[rows] if r == 0 else items_all.at[block, rows]
                    send(src, items_all.at[block, rows], z_send.at[way, half, r],
                         z_recv.at[way, half, r], {"rows_0": z_at(sign)})

    def x_forward(r):
        for way, sign in enumerate(signs):
            for half in (0, 1):
                length = chain_length(nx, way, half)
                place = users.at[rows_of(x_at(-sign * r) * nc + c, half)]
                if 1 <= r <= length:
                    arrived(place, x_recv.at[way, half, r - 1])
                if r < length:
                    send(place, place, x_send.at[way, half, r], x_recv.at[way, half, r],
                         {"rows_1": x_at(sign)})
                if 1 <= r <= length:
                    send(place, place, p_send.at[way, half, r], p_recv.at[way, half, r], partner)
                if r == 0 and way == 0:
                    send(place, place, p_send.at[way, half, 0], p_recv.at[way, half, 0], partner)

    def from_partner():
        for way, sign in enumerate(signs):
            for half in (0, 1):
                for r in range(1 if way else 0, chain_length(nx, way, half) + 1):
                    place = users.at[rows_of(x_at(-sign * r) * nc + 1 - c, half)]
                    arrived(place, p_recv.at[way, half, r])

    x_forward(0)
    z_forward(0)
    for step in range(1, peers):
        send(meta_all.at[me], meta_all.at[me], m_send.at[step], m_recv.at[step], peer(step))

    pre_keep[...] = pre.T

    for r in range(1, nx // 2 + 1):
        x_forward(r)
        if r == 1:
            z_forward(1)
    from_partner()

    def first_pass(chunk):
        own = items_all[chunk]
        items_turned[:, block_rows(chunk)] = own.T

        @pl.loop(0, peers)
        def _(k):
            s = contract(items_all[chunk], users[block_rows(k), :], (1, 1))
            top = jnp.max(s, axis=0, keepdims=True)
            p = jnp.exp(s - top)
            probs[chunk * peers + k] = p
            peaks[chunk, pl.ds(k, 1), :] = top
            sums[chunk, pl.ds(k, 1), :] = jnp.sum(p, axis=0, keepdims=True)

    first_pass(z)
    for r in range(1, nz // 2 + 1):
        if r > 1:
            z_forward(r)
        if r < nz // 2:
            first_pass(z_at(r))
            first_pass(z_at(-r))
        else:
            first_pass(z_at(r))

    tops = peaks[...]
    top = jnp.max(tops, axis=0)
    lses[me] = top + jnp.log(jnp.sum(sums[...] * jnp.exp(tops - top[None]), axis=0))
    for step in range(1, peers):
        send(lses.at[me], lses.at[me], l_send.at[step], l_recv.at[step], peer(step))
    for step in range(1, peers):
        arrived(meta_all.at[from_peer(step)], m_recv.at[step])
    for step in range(1, peers):
        arrived(lses.at[from_peer(step)], l_recv.at[step])
    parts = lses[...]
    top = jnp.max(parts, axis=0)
    total = top + jnp.log(jnp.sum(jnp.exp(parts - top[None]), axis=0))
    scale[...] = jnp.exp(tops - total[None])

    lines = lax.broadcasted_iota(jnp.int32, (size, size), 0)

    def second_pass(chunk):
        first = ((chunk * nx + x) * nc + c) * size

        @pl.loop(0, peers)
        def _(k):
            weight = meta_all[k, 0:1, :]
            target = meta_all[k, 1:2, :].astype(jnp.int32) - first
            t = probs[chunk * peers + k] * (scale[chunk, pl.ds(k, 1), :] * weight)
            t = jnp.where(lines == target, t - weight, t)
            ds[block_rows(chunk), block_rows(k)] = t.astype(BF16)

        gi_part[chunk] = jnp.dot(ds[block_rows(chunk), :], users[...], preferred_element_type=F32)

    def z_reduce(r, parts_of=((0, 0), (0, 1), (1, 0), (1, 1))):
        for way, half in parts_of:
            sign = signs[way]
            length = chain_length(nz, way, half)
            rows = pl.ds(half * half_size, half_size)
            dest = z_at(sign * (length - r))
            if 1 <= r <= length:
                land = z_land.at[way, half, r - 1]
                arrived(land, zr_recv.at[way, half, r - 1])
                if r < length:
                    land[...] += gi_part[dest, rows]
            if r < length:
                src = gi_part.at[dest, rows] if r == 0 else z_land.at[way, half, r - 1]
                send(src, z_land.at[way, half, r], zr_send.at[way, half, r],
                     zr_recv.at[way, half, r], {"rows_0": z_at(sign)})

    second_pass(z_at(nz // 2))
    z_reduce(0, ((0, 0), (1, 1)))
    second_pass(z_at(nz // 2 - 1))
    z_reduce(0, ((0, 1),))
    second_pass(z_at(1 - nz // 2))
    z_reduce(0, ((1, 0),))
    for r in range(nz // 2 - 2, 0, -1):
        second_pass(z_at(r))
        second_pass(z_at(-r))
    second_pass(z)

    def user_pass(k):
        gu_part[k] = jnp.dot(items_turned[...], ds[:, block_rows(k)], preferred_element_type=F32)

    z_reduce(1)
    for step in range(nx):
        k = x_at(step) * nc + 1 - c
        user_pass(k)
        send(gu_part.at[k], gu_pair.at[x_at(step)], d_send.at[step], d_recv.at[step], partner)
    for step in range(nx):
        user_pass(x_at(step) * nc + c)
    for step in range(nx):
        arrived(gu_pair.at[x_at(step)], d_recv.at[step])
        gu_pair[x_at(step)] += gu_part[x_at(step) * nc + c]

    def x_reduce(r):
        for way, sign in enumerate(signs):
            for half in (0, 1):
                length = chain_length(nx, way, half)
                rows = pl.ds(half * half_size, half_size)
                dest = x_at(sign * (length - r))
                if 1 <= r <= length:
                    land = x_land.at[way, half, r - 1]
                    arrived(land, xr_recv.at[way, half, r - 1])
                    if r < length:
                        land[...] += gu_pair[dest, rows]
                if r < length:
                    src = gu_pair.at[dest, rows] if r == 0 else x_land.at[way, half, r - 1]
                    send(src, x_land.at[way, half, r], xr_send.at[way, half, r],
                         xr_recv.at[way, half, r], {"rows_1": x_at(sign)})

    x_reduce(0)
    for r in range(1, nx // 2 + 1):
        if r + 1 <= nz // 2:
            z_reduce(r + 1)
        x_reduce(r)

    def collected(own, land, n):
        pieces = []
        for half in (0, 1):
            got = own[half * half_size : (half + 1) * half_size]
            for way in (0, 1):
                length = chain_length(n, way, half)
                if length:
                    got = got + land[way, half, length - 1]
            pieces.append(got)
        return jnp.concatenate(pieces, axis=0)

    gu = collected(gu_pair[x], x_land, nx).astype(BF16)
    pre = pre_keep[...]
    gate = jax.nn.sigmoid(pre)
    back = jnp.dot(w2_ref[...], gu, preferred_element_type=F32)
    grad_pre = (back * gate * (1.0 + pre * (1.0 - gate))).astype(BF16)
    df_ref[0] = jnp.dot(grad_pre, feat_ref[...], preferred_element_type=F32)
    df_ref[1] = jnp.dot(gu, hid_keep[...], preferred_element_type=F32)

    for r in range(nx // 2 + 2, nz // 2 + 1):
        z_reduce(r)
    gi_ref[...] = collected(gi_part[z], z_land, nz)
    for copy in pending:
        copy.wait_send()


def block_grads(features, w_first, w_second, items, meta):
    nz, nx, nc = (lax.axis_size(a) for a in ("rows_0", "rows_1", "rows_2"))
    size, width = items.shape
    peers = nx * nc
    vmem, dma = pltpu.VMEM, pltpu.SemaphoreType.DMA
    zh, xh = nz // 2, nx // 2
    return pl.pallas_call(
        functools.partial(block_kernel, nz, nx, nc),
        out_shape=(
            jax.ShapeDtypeStruct((size, width), F32),
            jax.ShapeDtypeStruct((2, width, width), F32),
        ),
        in_specs=[pl.BlockSpec(memory_space=vmem)] * 5,
        out_specs=[pl.BlockSpec(memory_space=vmem)] * 2,
        scratch_shapes=[
            vmem((peers * size, width), BF16),
            vmem((nz, size, width), BF16),
            vmem((width, nz * size), BF16),
            vmem((peers, 2, size), F32),
            vmem((nz, peers, size), F32),
            vmem((nz, peers, size), F32),
            vmem((peers, peers, size), F32),
            vmem((nz, peers, size), F32),
            vmem((nz * peers, size, size), F32),
            vmem((nz * size, peers * size), BF16),
            vmem((nz, size, width), F32),
            vmem((peers, width, size), F32),
            vmem((nx, width, size), F32),
            vmem((2, 2, zh, size // 2, width), F32),
            vmem((2, 2, xh, width // 2, size), F32),
            vmem((width, size), F32),
            vmem((size, width), BF16),
            dma((2, 2, zh)), dma((2, 2, zh)),
            dma((2, 2, xh)), dma((2, 2, xh)),
            dma((2, 2, xh + 1)), dma((2, 2, xh + 1)),
            dma((peers,)), dma((peers,)),
            dma((peers,)), dma((peers,)),
            dma((2, 2, zh)), dma((2, 2, zh)),
            dma((nx,)), dma((nx,)),
            dma((2, 2, xh)), dma((2, 2, xh)),
        ],
        compiler_params=pltpu.CompilerParams(
            collective_id=0, has_side_effects=True, vmem_limit_bytes=60 * 2**20
        ),
        cost_estimate=pl.CostEstimate(flops=7 * 10**9, bytes_accessed=2**20, transcendentals=2**22),
        name="block_grads",
    )(features, w_first, w_second, items, meta)


def cut_along(value, dim, count):
    before, after = (value.shape[:dim], value.shape[dim + 1 :])
    return jnp.moveaxis(value.reshape(*before, count, -1, *after), dim, 0)


def sum_at_owner(value, axis, dim):
    count = lax.axis_size(axis)
    tiles = lax.all_to_all(cut_along(value, dim, count), axis, 0, 0, tiled=True)
    return jnp.sum(tiles, axis=0)


def summed_rows(value, axes, dim):
    far, near = axes
    tiles = cut_along(value, dim, lax.axis_size(far))
    nearer = sum_at_owner(tiles, near, dim + 1)
    arrived = lax.all_to_all(nearer, far, split_axis=0, concat_axis=0, tiled=True)
    return arrived.sum(axis=0)


def padded_to(lines, count):
    spare = -lines.shape[0] % count
    if not spare:
        return lines
    return jnp.concatenate([lines, jnp.zeros((spare, *lines.shape[1:]), lines.dtype)])


def sent_to_all(value, axis):
    count = lax.axis_size(axis)
    return lax.all_to_all(
        jnp.broadcast_to(value[None], (count, *value.shape)), axis, 0, 0, tiled=True
    )


def joined_along(tiles, dim):
    shape = list(tiles.shape[1:])
    shape[dim] *= tiles.shape[0]
    return jnp.moveaxis(tiles, 0, dim).reshape(shape)


def gather_axes(value, axes, dim):
    far, near = axes
    tiles = sent_to_all(sent_to_all(value, far), near)
    return joined_along(tiles.swapaxes(0, 1).reshape(-1, *value.shape), dim)


def total_of(value, axes):
    own = summed_rows(padded_to(value, lax.axis_size(axes[0]) * lax.axis_size(axes[1])), axes, 0)
    whole = gather_axes(own, axes, 0)
    return whole[: len(value)].reshape(value.shape)


def in_one(arrays, axis):
    flat, at, done = (jnp.concatenate([a.reshape(-1) for a in arrays]), 0, [])
    total = total_of(flat, axis)
    for a in arrays:
        done.append(total[at : at + a.size].reshape(a.shape))
        at += a.size
    return tuple(done)


def one_exchange(value, axis, axes, splits, concats):
    sizes = [lax.axis_size(a) for a in axes]
    tiles = cut_along(value, splits[0], sizes[0])
    tiles = jnp.moveaxis(cut_along(tiles, splits[1] + 1, sizes[1]), 0, 1)
    inside = tiles.shape[2:]
    tiles = tiles.reshape(-1, *inside)
    tiles = lax.all_to_all(tiles, axis, split_axis=0, concat_axis=0, tiled=True)
    tiles = joined_along(tiles.reshape(*sizes, *inside), concats[0] + 1)
    return joined_along(tiles, concats[1])


def body(
    user_features, w_first, w_second, item_embed, example_weight, positive, item_owner, item_row
):
    own_items = item_embed[0]
    owners = item_owner[0, :, 0]
    item_rows = item_row[0]
    my_users, feature_width = own_items.shape
    peers = lax.axis_size(ROWS)
    groups = lax.axis_size("grp")
    capacity = max(2, 4 * my_users // peers)
    member = (owners[:, None] == lax.broadcasted_iota(jnp.int32, (1, peers), 1)).astype(jnp.int32)
    before = jnp.cumsum(member, axis=0) - member
    slot_rank = jnp.sum(before * member, axis=1)
    slots = owners * capacity + slot_rank
    send_rows = (
        jnp.full((peers * capacity,), -1.0, F32).at[slots].set(item_rows.astype(F32))
    )
    rows_wide = jnp.broadcast_to(send_rows.reshape(peers, capacity, 1), (peers, capacity, groups))
    got_rows = one_exchange(rows_wide, ROWS_GRP, (ROWS, "grp"), (0, 2), (0, 1))
    meta = jnp.stack([example_weight[0], positive[0].astype(F32)])
    grad_item, tower = block_grads(user_features[0], w_first, w_second, own_items, meta)
    send_grad = jnp.zeros((peers * capacity, feature_width), BF16).at[slots].set(grad_item.astype(BF16))
    send_grad = send_grad.reshape(peers, capacity, feature_width)
    got_grad = one_exchange(send_grad, ROWS_GRP, (ROWS, "grp"), (0, 2), (0, 1))
    (summed,) = in_one((tower,), (("rows_0", "rows_1"), ("rows_2", "grp")))
    share_width = feature_width // groups
    table_rows = got_rows.reshape(-1).astype(jnp.int32)
    table_rows = jnp.where(table_rows >= 0, table_rows, ITEMS_DEV)
    grad_table = (
        jnp.zeros((ITEMS_DEV, share_width), F32)
        .at[table_rows]
        .add(got_grad.reshape(-1, share_width).astype(F32), mode="drop")
    )
    return (summed[0].T, summed[1].T, grad_table)


def solution(mesh):
    torus = Mesh(
        mesh.devices.reshape(8, 4, 2, mesh.shape["grp"]), ("rows_0", "rows_1", "rows_2", "grp")
    )
    placed = (
        P("grp", ROWS, None),
        P(),
        P(),
        P("grp", ROWS, None),
        P("grp", ROWS),
        P("grp", ROWS),
        P("grp", ROWS, None),
        P("grp", ROWS),
    )
    return jax.shard_map(
        body, mesh=torus, in_specs=placed, out_specs=(P(), P(), P(ROWS, "grp")), check_vma=False
    )
```

```python
import functools
import jax
import jax.numpy as jnp
from jax import lax
from jax.experimental import pallas as pl
from jax.experimental.pallas import tpu as pltpu
from jax.sharding import Mesh
from jax.sharding import PartitionSpec as P

ITEMS_DEV = 4096
ROWS = ("rows_0", "rows_1", "rows_2")
MESH = pl.DeviceIdType.MESH
F32 = jnp.float32
BF16 = jnp.bfloat16


def chain_length(n, way, half):
    return n // 2 if (way == 0) == (half == 0) else n // 2 - 1


def contract(left, right, dims):
    return lax.dot_general(left, right, ((dims[:1], dims[1:]), ((), ())), preferred_element_type=F32)


def block_kernel(
    nz, nx, nc, ny, feat_ref, w1_ref, w2_ref, items_ref, meta_ref, pairs_ref, got_ref, ids_ref, tower_ref,
    users, items_all, items_turned, meta_all, peaks, sums, lses, scale, probs, ds,
    gi_part, gu_part, gu_pair, z_land, x_land, pre_keep, hid_keep,
    z_send, z_recv, x_send, x_recv, p_send, p_recv, m_send, m_recv, l_send, l_recv,
    zr_send, zr_recv, d_send, d_recv, xr_send, xr_recv,
    pairs_all, slots_keep, ids_out, share_out, share_in, slotted,
    df_keep, df_pair, y_part, y_land, p_part, p_land,
    i_send, i_recv, n_send, n_recv, s_send, s_recv, e_send, e_recv,
    ac_send, ac_recv, ay_send, ay_recv, ap_send, ap_recv,
    gp_send, gp_recv, gy_send, gy_recv, gc_send, gc_recv,
):
    z, x, c = lax.axis_index("rows_0"), lax.axis_index("rows_1"), lax.axis_index("rows_2")
    y = lax.axis_index("grp")
    size = items_ref.shape[0]
    half_size = size // 2
    peers = nx * nc
    me = x * nc + c
    signs = (1, -1)

    def z_at(step):
        return lax.rem(z + step + nz, nz)

    def x_at(step):
        return lax.rem(x + step + nx, nx)

    def peer(step):
        dx, dc = divmod(step, nc)
        return {"rows_1": x_at(dx), "rows_2": lax.rem(c + dc, nc)}

    def from_peer(step):
        dx, dc = divmod(step, nc)
        return x_at(-dx) * nc + lax.rem(c + nc - dc, nc)

    partner = {"rows_2": 1 - c}
    pending = []

    def send(src, dst, send_sem, recv_sem, where):
        copy = pltpu.make_async_remote_copy(
            src_ref=src, dst_ref=dst, send_sem=send_sem, recv_sem=recv_sem,
            device_id=where, device_id_type=MESH,
        )
        copy.start()
        pending.append(copy)

    def arrived(ref, recv_sem):
        pltpu.make_async_copy(ref, ref, recv_sem).wait()

    barrier = pltpu.get_barrier_semaphore()
    plane = nz * peers
    here = z * peers + me
    tiles = nz * nx
    tile = z * nx + x

    def far(step):
        to_z = lax.rem(z + step // peers, nz)
        to_x = lax.rem(x + (step % peers) // nc, nx)
        to_c = lax.rem(c + step % nc, nc)
        return {"rows_0": to_z, "rows_1": to_x, "rows_2": to_c}, (to_z * nx + to_x) * nc + to_c

    def from_far(step):
        of_z = lax.rem(z + nz - step // peers, nz)
        of_x = lax.rem(x + nx - (step % peers) // nc, nx)
        of_c = lax.rem(c + nc - step % nc, nc)
        return (of_z * nx + of_x) * nc + of_c

    def far_tile(step):
        to_z, to_x = lax.rem(z + step // nx, nz), lax.rem(x + step % nx, nx)
        return {"rows_0": to_z, "rows_1": to_x}, to_z * nx + to_x

    def from_far_tile(step):
        return lax.rem(z + nz - step // nx, nz) * nx + lax.rem(x + nx - step % nx, nx)

    def y_at(step):
        return lax.rem(y + step + ny, ny)

    def send_plainly(src, dst, send_sem, recv_sem, where):
        pltpu.make_async_remote_copy(
            src_ref=src, dst_ref=dst, send_sem=send_sem, recv_sem=recv_sem,
            device_id=where, device_id_type=MESH,
        ).start()

    @pl.loop(1, plane)
    def _(step):
        pl.semaphore_signal(barrier, inc=1, device_id=far(step)[0], device_id_type=MESH)

    for step in range(1, ny):
        pl.semaphore_signal(barrier, inc=1, device_id={"grp": y_at(step)}, device_id_type=MESH)

    def rows_of(block, half):
        return pl.ds(pl.multiple_of(block * size + half * half_size, half_size), half_size)

    def block_rows(block):
        return pl.ds(pl.multiple_of(block * size, size), size)

    pre = jnp.dot(feat_ref[...], w1_ref[...], preferred_element_type=F32)
    hidden = (pre * jax.nn.sigmoid(pre)).astype(BF16)
    hid_keep[...] = hidden
    users[block_rows(me), :] = jnp.dot(hidden, w2_ref[...], preferred_element_type=F32).astype(BF16)
    items_all[z] = items_ref[...]
    meta_all[me] = meta_ref[...]

    pairs_all[y] = pairs_ref[...]
    pl.semaphore_wait(barrier, plane - 1 + ny - 1)

    def z_forward(r):
        for way, sign in enumerate(signs):
            for half in (0, 1):
                length = chain_length(nz, way, half)
                rows = pl.ds(half * half_size, half_size)
                if 1 <= r <= length:
                    arrived(items_all.at[z_at(-sign * r), rows], z_recv.at[way, half, r - 1])
                if r < length:
                    block = z_at(-sign * r)
                    src = items_ref.at[rows] if r == 0 else items_all.at[block, rows]
                    send(src, items_all.at[block, rows], z_send.at[way, half, r],
                         z_recv.at[way, half, r], {"rows_0": z_at(sign)})

    def x_forward(r):
        for way, sign in enumerate(signs):
            for half in (0, 1):
                length = chain_length(nx, way, half)
                place = users.at[rows_of(x_at(-sign * r) * nc + c, half)]
                if 1 <= r <= length:
                    arrived(place, x_recv.at[way, half, r - 1])
                if r < length:
                    send(place, place, x_send.at[way, half, r], x_recv.at[way, half, r],
                         {"rows_1": x_at(sign)})
                if 1 <= r <= length:
                    send(place, place, p_send.at[way, half, r], p_recv.at[way, half, r], partner)
                if r == 0 and way == 0:
                    send(place, place, p_send.at[way, half, 0], p_recv.at[way, half, 0], partner)

    def from_partner():
        for way, sign in enumerate(signs):
            for half in (0, 1):
                for r in range(1 if way else 0, chain_length(nx, way, half) + 1):
                    place = users.at[rows_of(x_at(-sign * r) * nc + 1 - c, half)]
                    arrived(place, p_recv.at[way, half, r])

    x_forward(0)
    z_forward(0)
    for step in range(1, peers):
        send(meta_all.at[me], meta_all.at[me], m_send.at[step], m_recv.at[step], peer(step))

    for step in range(1, ny):
        send(pairs_all.at[y], pairs_all.at[y], i_send.at[step], i_recv.at[step],
             {"grp": y_at(step)})

    pre_keep[...] = pre.T

    cap = got_ref.shape[2]
    share = got_ref.shape[3] // 2

    def name_slots():
        earlier = (
            lax.broadcasted_iota(jnp.int32, (size, size), 0)
            < lax.broadcasted_iota(jnp.int32, (size, size), 1)
        ).astype(BF16)
        owner_lines = lax.broadcasted_iota(jnp.int32, (plane, size), 0)
        rank_lines = lax.broadcasted_iota(jnp.int32, (cap, size), 0)
        pieces, most = [], None
        for g in range(ny):
            owner = pairs_all[g, 0:1, :].astype(jnp.int32)
            row = pairs_all[g, 1:2, :]
            member = (owner_lines == owner).astype(F32)
            before = jnp.dot(member.astype(BF16), earlier, preferred_element_type=F32)
            rank = jnp.sum(before * member, axis=0, keepdims=True).astype(jnp.int32)
            slots_keep[g] = owner * cap + rank
            at_rank = (rank_lines == rank).astype(BF16)
            high = jnp.floor(row * (1.0 / 64.0))
            low = row - 64.0 * high
            found = contract(member.astype(BF16), at_rank, (1, 1))
            ids = 64.0 * contract((member * high).astype(BF16), at_rank, (1, 1)) + contract(
                (member * low).astype(BF16), at_rank, (1, 1)
            )
            pieces.append(jnp.where(found > 0.5, ids, float(ITEMS_DEV)))
            count = jnp.sum(member, axis=1, keepdims=True)
            most = count if most is None else jnp.maximum(most, count)
        spare = ids_ref.shape[2] - ny * cap
        pieces.append(jnp.broadcast_to(most, (plane, spare)))
        named = jnp.concatenate(pieces, axis=1).astype(jnp.int32)
        ids_out[...] = named.reshape(ids_out.shape)

    for r in range(1, nx // 2 + 1):
        x_forward(r)
        if r == 1:
            z_forward(1)
            for step in range(1, ny):
                arrived(pairs_all.at[y_at(-step)], i_recv.at[step])
            name_slots()
    from_partner()

    def first_pass(chunk):
        own = items_all[chunk]
        items_turned[:, block_rows(chunk)] = own.T

        @pl.loop(0, peers)
        def _(k):
            s = contract(items_all[chunk], users[block_rows(k), :], (1, 1))
            top = jnp.max(s, axis=0, keepdims=True)
            p = jnp.exp(s - top)
            probs[chunk * peers + k] = p
            peaks[chunk, pl.ds(k, 1), :] = top
            sums[chunk, pl.ds(k, 1), :] = jnp.sum(p, axis=0, keepdims=True)

    first_pass(z)

    @pl.loop(1, plane)
    def _(step):
        where, there = far(step)
        send_plainly(ids_out.at[there], ids_ref.at[here], n_send.at[step], n_recv.at[step], where)

    ids_ref[here] = ids_out[here]
    for r in range(1, nz // 2 + 1):
        if r > 1:
            z_forward(r)
        if r < nz // 2:
            first_pass(z_at(r))
            first_pass(z_at(-r))
        else:
            first_pass(z_at(r))

    tops = peaks[...]
    top = jnp.max(tops, axis=0)
    lses[me] = top + jnp.log(jnp.sum(sums[...] * jnp.exp(tops - top[None]), axis=0))
    for step in range(1, peers):
        send(lses.at[me], lses.at[me], l_send.at[step], l_recv.at[step], peer(step))
    for step in range(1, peers):
        arrived(meta_all.at[from_peer(step)], m_recv.at[step])
    for step in range(1, peers):
        arrived(lses.at[from_peer(step)], l_recv.at[step])
    parts = lses[...]
    top = jnp.max(parts, axis=0)
    total = top + jnp.log(jnp.sum(jnp.exp(parts - top[None]), axis=0))
    scale[...] = jnp.exp(tops - total[None])

    lines = lax.broadcasted_iota(jnp.int32, (size, size), 0)

    def second_pass(chunk):
        first = ((chunk * nx + x) * nc + c) * size

        @pl.loop(0, peers)
        def _(k):
            weight = meta_all[k, 0:1, :]
            target = meta_all[k, 1:2, :].astype(jnp.int32) - first
            t = probs[chunk * peers + k] * (scale[chunk, pl.ds(k, 1), :] * weight)
            t = jnp.where(lines == target, t - weight, t)
            ds[block_rows(chunk), block_rows(k)] = t.astype(BF16)

        gi_part[chunk] = jnp.dot(ds[block_rows(chunk), :], users[...], preferred_element_type=F32)

    def z_reduce(r, parts_of=((0, 0), (0, 1), (1, 0), (1, 1))):
        for way, half in parts_of:
            sign = signs[way]
            length = chain_length(nz, way, half)
            rows = pl.ds(half * half_size, half_size)
            dest = z_at(sign * (length - r))
            if 1 <= r <= length:
                land = z_land.at[way, half, r - 1]
                arrived(land, zr_recv.at[way, half, r - 1])
                if r < length:
                    land[...] += gi_part[dest, rows]
            if r < length:
                src = gi_part.at[dest, rows] if r == 0 else z_land.at[way, half, r - 1]
                send(src, z_land.at[way, half, r], zr_send.at[way, half, r],
                     zr_recv.at[way, half, r], {"rows_0": z_at(sign)})

    second_pass(z_at(nz // 2))
    z_reduce(0, ((0, 0), (1, 1)))
    second_pass(z_at(nz // 2 - 1))
    z_reduce(0, ((0, 1),))
    second_pass(z_at(1 - nz // 2))
    z_reduce(0, ((1, 0),))
    for r in range(nz // 2 - 2, 0, -1):
        second_pass(z_at(r))
        second_pass(z_at(-r))
    second_pass(z)

    def user_pass(k):
        gu_part[k] = jnp.dot(items_turned[...], ds[:, block_rows(k)], preferred_element_type=F32)

    z_reduce(1)
    for step in range(nx):
        k = x_at(step) * nc + 1 - c
        user_pass(k)
        send(gu_part.at[k], gu_pair.at[x_at(step)], d_send.at[step], d_recv.at[step], partner)
    for step in range(nx):
        user_pass(x_at(step) * nc + c)
    for step in range(nx):
        arrived(gu_pair.at[x_at(step)], d_recv.at[step])
        gu_pair[x_at(step)] += gu_part[x_at(step) * nc + c]

    def x_reduce(r):
        for way, sign in enumerate(signs):
            for half in (0, 1):
                length = chain_length(nx, way, half)
                rows = pl.ds(half * half_size, half_size)
                dest = x_at(sign * (length - r))
                if 1 <= r <= length:
                    land = x_land.at[way, half, r - 1]
                    arrived(land, xr_recv.at[way, half, r - 1])
                    if r < length:
                        land[...] += gu_pair[dest, rows]
                if r < length:
                    src = gu_pair.at[dest, rows] if r == 0 else x_land.at[way, half, r - 1]
                    send(src, x_land.at[way, half, r], xr_send.at[way, half, r],
                         xr_recv.at[way, half, r], {"rows_1": x_at(sign)})

    x_reduce(0)
    for r in range(1, nx // 2 + 1):
        if r + 1 <= nz // 2:
            z_reduce(r + 1)
        x_reduce(r)

    def collected(own, land, n):
        pieces = []
        for half in (0, 1):
            got = own[half * half_size : (half + 1) * half_size]
            for way in (0, 1):
                length = chain_length(n, way, half)
                if length:
                    got = got + land[way, half, length - 1]
            pieces.append(got)
        return jnp.concatenate(pieces, axis=0)

    gu = collected(gu_pair[x], x_land, nx).astype(BF16)
    pre = pre_keep[...]
    gate = jax.nn.sigmoid(pre)
    back = jnp.dot(w2_ref[...], gu, preferred_element_type=F32)
    grad_pre = (back * gate * (1.0 + pre * (1.0 - gate))).astype(BF16)
    df_keep[0] = jnp.dot(grad_pre, feat_ref[...], preferred_element_type=F32)
    df_keep[1] = jnp.dot(gu, hid_keep[...], preferred_element_type=F32)

    send(df_keep.at[1 - c], df_pair, ac_send, ac_recv, partner)
    arrived(df_pair, ac_recv)
    y_part[...] = (df_keep[c] + df_pair[...]).reshape(y_part.shape)
    for step in range(1, ny):
        send(y_part.at[y_at(step)], y_land.at[step - 1], ay_send.at[step], ay_recv.at[step],
             {"grp": y_at(step)})

    for r in range(nx // 2 + 2, nz // 2 + 1):
        z_reduce(r)
    gi = collected(gi_part[z], z_land, nz).astype(BF16)

    for to in range(ny):
        cols = slice(to * share, (to + 1) * share)
        share_out[to] = jnp.concatenate([gi[:half_size, cols], gi[half_size:, cols]], axis=1)
    for step in range(1, ny):
        send(share_out.at[y_at(step)], share_in.at[y], s_send.at[step], s_recv.at[step],
             {"grp": y_at(step)})
    share_in[y] = share_out[y]

    whole = y_part[y]
    for step in range(1, ny):
        arrived(y_land.at[step - 1], ay_recv.at[step])
        whole = whole + y_land[step - 1]
    p_part[...] = whole.reshape(p_part.shape)

    @pl.loop(1, tiles)
    def _(step):
        where, there = far_tile(step)
        send_plainly(p_part.at[there], p_land.at[step], ap_send.at[step], ap_recv.at[step], where)

    for step in range(1, ny):
        arrived(share_in.at[y_at(-step)], s_recv.at[step])
    slot_lines = lax.broadcasted_iota(jnp.int32, (plane * cap, size), 0)
    for pair in range(ny // 2):
        sides = []
        for g in (2 * pair, 2 * pair + 1):
            chosen = (slot_lines == slots_keep[g]).astype(BF16)
            packed = share_in[g]
            data = jnp.concatenate([packed[:, :share], packed[:, share:]], axis=0)
            sides.append(jnp.dot(chosen, data, preferred_element_type=F32))
        both = jnp.concatenate(sides, axis=1).astype(BF16)
        slotted[:, pair] = both.reshape(plane, cap, 2 * share)
    got_ref[here] = slotted[here]

    def exchange(first, last):
        @pl.loop(first, last)
        def _(step):
            where, there = far(step)
            send_plainly(slotted.at[there], got_ref.at[here], e_send.at[step], e_recv.at[step],
                         where)

    exchange(1, plane // 2)
    p_land[0] = p_part[tile]

    @pl.loop(1, tiles)
    def _(step):
        arrived(p_land.at[step], ap_recv.at[step])

    own = tower_ref.at[c, y, tile]
    own[...] = jnp.sum(p_land[...], axis=0)

    @pl.loop(1, tiles)
    def _(step):
        where, _ = far_tile(step)
        send_plainly(own, own, gp_send.at[step], gp_recv.at[step], where)

    exchange(plane // 2, plane)

    @pl.loop(1, tiles)
    def _(step):
        arrived(tower_ref.at[c, y, from_far_tile(step)], gp_recv.at[step])

    for step in range(1, ny):
        send(tower_ref.at[c, y], tower_ref.at[c, y], gy_send.at[step], gy_recv.at[step],
             {"grp": y_at(step)})
    for step in range(1, ny):
        arrived(tower_ref.at[c, y_at(-step)], gy_recv.at[step])
    send(tower_ref.at[c], tower_ref.at[c], gc_send, gc_recv, partner)

    @pl.loop(1, plane)
    def _(step):
        arrived(ids_ref.at[from_far(step)], n_recv.at[step])
        arrived(got_ref.at[from_far(step)], e_recv.at[step])

    arrived(tower_ref.at[1 - c], gc_recv)
    for copy in pending:
        copy.wait_send()

    @pl.loop(1, plane)
    def _(step):
        arrived(ids_out.at[0], n_send.at[step])
        arrived(slotted.at[0], e_send.at[step])

    @pl.loop(1, tiles)
    def _(step):
        arrived(p_part.at[0], ap_send.at[step])
        arrived(p_part.at[0], gp_send.at[step])


def block_grads(features, w_first, w_second, items, meta, pairs):
    nz, nx, nc = (lax.axis_size(a) for a in ROWS)
    ny = lax.axis_size("grp")
    size, width = items.shape
    peers = nx * nc
    plane, tiles = nz * peers, nz * nx
    cap = max(2, 4 * size // plane)
    share = width // ny
    vmem, dma = pltpu.VMEM, pltpu.SemaphoreType.DMA
    zh, xh = nz // 2, nx // 2
    lane = ny * cap + 64
    tower = (nc, ny, tiles, width // ny // tiles, width)
    return pl.pallas_call(
        functools.partial(block_kernel, nz, nx, nc, ny),
        out_shape=(
            jax.ShapeDtypeStruct((plane, ny // 2, cap, 2 * share), BF16),
            jax.ShapeDtypeStruct((plane, 1, lane), jnp.int32),
            jax.ShapeDtypeStruct(tower, F32),
        ),
        in_specs=[pl.BlockSpec(memory_space=vmem)] * 6,
        out_specs=[pl.BlockSpec(memory_space=vmem)] * 3,
        scratch_shapes=[
            vmem((peers * size, width), BF16),
            vmem((nz, size, width), BF16),
            vmem((width, nz * size), BF16),
            vmem((peers, 2, size), F32),
            vmem((nz, peers, size), F32),
            vmem((nz, peers, size), F32),
            vmem((peers, peers, size), F32),
            vmem((nz, peers, size), F32),
            vmem((nz * peers, size, size), F32),
            vmem((nz * size, peers * size), BF16),
            vmem((nz, size, width), F32),
            vmem((peers, width, size), F32),
            vmem((nx, width, size), F32),
            vmem((2, 2, zh, size // 2, width), F32),
            vmem((2, 2, xh, width // 2, size), F32),
            vmem((width, size), F32),
            vmem((size, width), BF16),
            dma((2, 2, zh)), dma((2, 2, zh)),
            dma((2, 2, xh)), dma((2, 2, xh)),
            dma((2, 2, xh + 1)), dma((2, 2, xh + 1)),
            dma((peers,)), dma((peers,)),
            dma((peers,)), dma((peers,)),
            dma((2, 2, zh)), dma((2, 2, zh)),
            dma((nx,)), dma((nx,)),
            dma((2, 2, xh)), dma((2, 2, xh)),
            vmem((ny, 2, size), F32),
            vmem((ny, 1, size), jnp.int32),
            vmem((plane, 1, lane), jnp.int32),
            vmem((ny, size // 2, 2 * share), BF16),
            vmem((ny, size // 2, 2 * share), BF16),
            vmem((plane, ny // 2, cap, 2 * share), BF16),
            vmem((2, width, width), F32),
            vmem((width, width), F32),
            vmem((ny, width // ny, width), F32),
            vmem((ny - 1, width // ny, width), F32),
            vmem(tower[2:], F32),
            vmem(tower[2:], F32),
            dma((ny,)), dma((ny,)),
            dma((plane,)), dma((plane,)),
            dma((ny,)), dma((ny,)),
            dma((plane,)), dma((plane,)),
            dma, dma,
            dma((ny,)), dma((ny,)),
            dma((tiles,)), dma((tiles,)),
            dma((tiles,)), dma((tiles,)),
            dma((ny,)), dma((ny,)),
            dma, dma,
        ],
        compiler_params=pltpu.CompilerParams(
            collective_id=0, has_side_effects=True, vmem_limit_bytes=60 * 2**20
        ),
        cost_estimate=pl.CostEstimate(flops=7 * 10**9, bytes_accessed=2**20, transcendentals=2**22),
        name="block_grads",
    )(features, w_first, w_second, items, meta, pairs)


def table_kernel(ids_ref, got_ref, out_ref, lines, *tables):
    sources, pairs, cap, lanes = got_ref.shape
    share = lanes // 2
    count = out_ref.shape[0]
    lines[...] = got_ref[...].astype(F32).reshape(lines.shape)
    for table in tables:
        table[...] = jnp.zeros_like(table)

    @pl.loop(0, sources)
    def _(source):
        @pl.loop(0, ids_ref[source, 2 * pairs * cap])
        def _(slot):
            for pair in range(pairs):
                line = lines[pl.ds((source * pairs + pair) * cap + slot, 1), :]
                for side in (0, 1):
                    g = 2 * pair + side
                    at = pl.ds(ids_ref[source, g * cap + slot], 1)
                    tables[g][at, :] += line

    even = sum(t[:count, :] for t in tables[0::2])
    odd = sum(t[:count, :] for t in tables[1::2])
    out_ref[...] = even[:, :share] + odd[:, share:]


def table_grads(ids, got):
    sources, pairs, cap, lanes = got.shape
    vmem = pltpu.VMEM
    return pl.pallas_call(
        table_kernel,
        out_shape=jax.ShapeDtypeStruct((ITEMS_DEV, lanes // 2), F32),
        in_specs=[pl.BlockSpec(memory_space=pltpu.SMEM), pl.BlockSpec(memory_space=vmem)],
        out_specs=pl.BlockSpec(memory_space=vmem),
        scratch_shapes=[vmem((sources * pairs * cap, lanes), F32)]
        + [vmem((ITEMS_DEV + 8, lanes), F32)] * (2 * pairs),
        compiler_params=pltpu.CompilerParams(vmem_limit_bytes=40 * 2**20),
        name="table_grads",
    )(ids, got)


def body(
    user_features, w_first, w_second, item_embed, example_weight, positive, item_owner, item_row
):
    width = w_second.shape[1]
    meta = jnp.stack([example_weight[0], positive[0].astype(F32)])
    pairs = jnp.stack([item_owner[0, :, 0].astype(F32), item_row[0].astype(F32)])
    got, ids, tower = block_grads(
        user_features[0], w_first, w_second, item_embed[0], meta, pairs
    )
    grad_table = table_grads(ids.reshape(ids.shape[0], -1), got)
    tower = tower.reshape(2, width, width)
    return (tower[0].T, tower[1].T, grad_table)


def solution(mesh):
    torus = Mesh(
        mesh.devices.reshape(8, 4, 2, mesh.shape["grp"]), ("rows_0", "rows_1", "rows_2", "grp")
    )
    placed = (
        P("grp", ROWS, None),
        P(),
        P(),
        P("grp", ROWS, None),
        P("grp", ROWS),
        P("grp", ROWS),
        P("grp", ROWS, None),
        P("grp", ROWS),
    )
    return jax.shard_map(
        body, mesh=torus, in_specs=placed, out_specs=(P(), P(), P(ROWS, "grp")), check_vma=False
    )
```

```python
import functools
import jax
import jax.numpy as jnp
from jax import lax
from jax.experimental import pallas as pl
from jax.experimental.pallas import tpu as pltpu
from jax.sharding import Mesh
from jax.sharding import PartitionSpec as P

ITEMS_DEV = 4096
ROWS = ("rows_0", "rows_1", "rows_2")
MESH = pl.DeviceIdType.MESH
F32 = jnp.float32
BF16 = jnp.bfloat16


def chain_length(n, way, half):
    return n // 2 if (way == 0) == (half == 0) else n // 2 - 1


def contract(left, right, dims):
    return lax.dot_general(left, right, ((dims[:1], dims[1:]), ((), ())), preferred_element_type=F32)


def block_kernel(
    nz, nx, nc, ny, feat_ref, w1_ref, w2_ref, items_ref, weight_ref, target_ref, owner_ref, row_ref,
    got_ref, ids_ref, tower_ref,
    users, items_all, items_turned, meta_all, peaks, sums, lses, scale, probs, ds,
    gi_part, gu_part, gu_pair, z_land, x_land, pre_keep, hid_keep,
    z_send, z_recv, x_send, x_recv, p_send, p_recv, m_send, m_recv, l_send, l_recv,
    zr_send, zr_recv, d_send, d_recv, xr_send, xr_recv,
    pairs_all, slots_keep, ids_out, share_out, share_in, slotted,
    df_keep, df_pair, y_part, y_land, p_part, p_land,
    i_send, i_recv, n_send, n_recv, s_send, s_recv, e_send, e_recv,
    ac_send, ac_recv, ay_send, ay_recv, ap_send, ap_recv,
    gp_send, gp_recv, gy_send, gy_recv, gc_send, gc_recv,
):
    z, x, c = lax.axis_index("rows_0"), lax.axis_index("rows_1"), lax.axis_index("rows_2")
    y = lax.axis_index("grp")
    size = items_ref.shape[0]
    half_size = size // 2
    peers = nx * nc
    me = x * nc + c
    signs = (1, -1)

    def z_at(step):
        return lax.rem(z + step + nz, nz)

    def x_at(step):
        return lax.rem(x + step + nx, nx)

    def peer(step):
        dx, dc = divmod(step, nc)
        return {"rows_1": x_at(dx), "rows_2": lax.rem(c + dc, nc)}

    def from_peer(step):
        dx, dc = divmod(step, nc)
        return x_at(-dx) * nc + lax.rem(c + nc - dc, nc)

    partner = {"rows_2": 1 - c}
    pending = []

    def send(src, dst, send_sem, recv_sem, where):
        copy = pltpu.make_async_remote_copy(
            src_ref=src, dst_ref=dst, send_sem=send_sem, recv_sem=recv_sem,
            device_id=where, device_id_type=MESH,
        )
        copy.start()
        pending.append(copy)

    def arrived(ref, recv_sem):
        pltpu.make_async_copy(ref, ref, recv_sem).wait()

    barrier = pltpu.get_barrier_semaphore()
    plane = nz * peers
    here = z * peers + me
    tiles = nz * nx
    tile = z * nx + x

    def far(step):
        to_z = lax.rem(z + step // peers, nz)
        to_x = lax.rem(x + (step % peers) // nc, nx)
        to_c = lax.rem(c + step % nc, nc)
        return {"rows_0": to_z, "rows_1": to_x, "rows_2": to_c}, (to_z * nx + to_x) * nc + to_c

    def from_far(step):
        of_z = lax.rem(z + nz - step // peers, nz)
        of_x = lax.rem(x + nx - (step % peers) // nc, nx)
        of_c = lax.rem(c + nc - step % nc, nc)
        return (of_z * nx + of_x) * nc + of_c

    def far_tile(step):
        to_z, to_x = lax.rem(z + step // nx, nz), lax.rem(x + step % nx, nx)
        return {"rows_0": to_z, "rows_1": to_x}, to_z * nx + to_x

    def from_far_tile(step):
        return lax.rem(z + nz - step // nx, nz) * nx + lax.rem(x + nx - step % nx, nx)

    def y_at(step):
        return lax.rem(y + step + ny, ny)

    def send_plainly(src, dst, send_sem, recv_sem, where):
        pltpu.make_async_remote_copy(
            src_ref=src, dst_ref=dst, send_sem=send_sem, recv_sem=recv_sem,
            device_id=where, device_id_type=MESH,
        ).start()

    @pl.loop(1, plane)
    def _(step):
        pl.semaphore_signal(barrier, inc=1, device_id=far(step)[0], device_id_type=MESH)

    for step in range(1, ny):
        pl.semaphore_signal(barrier, inc=1, device_id={"grp": y_at(step)}, device_id_type=MESH)

    def rows_of(block, half):
        return pl.ds(pl.multiple_of(block * size + half * half_size, half_size), half_size)

    def block_rows(block):
        return pl.ds(pl.multiple_of(block * size, size), size)

    with jax.named_scope("tower"):
        pre = jnp.dot(feat_ref[...], w1_ref[...], preferred_element_type=F32)
        hidden = (pre * jax.nn.sigmoid(pre)).astype(BF16)
        hid_keep[...] = hidden
        users[block_rows(me), :] = jnp.dot(hidden, w2_ref[...], preferred_element_type=F32).astype(BF16)
        items_all[z] = items_ref[...]
        meta_all[me, 0:1, :] = weight_ref[...]
        meta_all[me, 1:2, :] = target_ref[...].astype(F32)

        pairs_all[y, 0:1, :] = owner_ref[...].astype(F32)
        pairs_all[y, 1:2, :] = row_ref[...].astype(F32)
    with jax.named_scope("barrier"):
        pl.semaphore_wait(barrier, plane - 1 + ny - 1)

    def z_forward(r):
        for way, sign in enumerate(signs):
            for half in (0, 1):
                length = chain_length(nz, way, half)
                rows = pl.ds(half * half_size, half_size)
                if 1 <= r <= length:
                    arrived(items_all.at[z_at(-sign * r), rows], z_recv.at[way, half, r - 1])
                if r < length:
                    block = z_at(-sign * r)
                    src = items_ref.at[rows] if r == 0 else items_all.at[block, rows]
                    send(src, items_all.at[block, rows], z_send.at[way, half, r],
                         z_recv.at[way, half, r], {"rows_0": z_at(sign)})

    def x_forward(r):
        for way, sign in enumerate(signs):
            for half in (0, 1):
                length = chain_length(nx, way, half)
                place = users.at[rows_of(x_at(-sign * r) * nc + c, half)]
                if 1 <= r <= length:
                    arrived(place, x_recv.at[way, half, r - 1])
                if r < length:
                    send(place, place, x_send.at[way, half, r], x_recv.at[way, half, r],
                         {"rows_1": x_at(sign)})
                if 1 <= r <= length:
                    send(place, place, p_send.at[way, half, r], p_recv.at[way, half, r], partner)
                if r == 0 and way == 0:
                    send(place, place, p_send.at[way, half, 0], p_recv.at[way, half, 0], partner)

    def from_partner():
        for way, sign in enumerate(signs):
            for half in (0, 1):
                for r in range(1 if way else 0, chain_length(nx, way, half) + 1):
                    place = users.at[rows_of(x_at(-sign * r) * nc + 1 - c, half)]
                    arrived(place, p_recv.at[way, half, r])

    with jax.named_scope("start"):
        x_forward(0)
        z_forward(0)
        for step in range(1, peers):
            send(meta_all.at[me], meta_all.at[me], m_send.at[step], m_recv.at[step], peer(step))

        for step in range(1, ny):
            send(pairs_all.at[y], pairs_all.at[y], i_send.at[step], i_recv.at[step],
                 {"grp": y_at(step)})

        pre_keep[...] = pre.T

    cap = got_ref.shape[2]
    share = got_ref.shape[3] // 2

    def name_slots():
        earlier = (
            lax.broadcasted_iota(jnp.int32, (size, size), 0)
            < lax.broadcasted_iota(jnp.int32, (size, size), 1)
        ).astype(BF16)
        owner_lines = lax.broadcasted_iota(jnp.int32, (plane, size), 0)
        rank_lines = lax.broadcasted_iota(jnp.int32, (cap, size), 0)
        pieces, most = [], None
        for g in range(ny):
            owner = pairs_all[g, 0:1, :].astype(jnp.int32)
            row = pairs_all[g, 1:2, :]
            member = (owner_lines == owner).astype(F32)
            before = jnp.dot(member.astype(BF16), earlier, preferred_element_type=F32)
            rank = jnp.sum(before * member, axis=0, keepdims=True).astype(jnp.int32)
            slots_keep[g] = owner * cap + rank
            at_rank = (rank_lines == rank).astype(BF16)
            high = jnp.floor(row * (1.0 / 64.0))
            low = row - 64.0 * high
            found = contract(member.astype(BF16), at_rank, (1, 1))
            ids = 64.0 * contract((member * high).astype(BF16), at_rank, (1, 1)) + contract(
                (member * low).astype(BF16), at_rank, (1, 1)
            )
            pieces.append(jnp.where(found > 0.5, ids, float(ITEMS_DEV)))
            count = jnp.sum(member, axis=1, keepdims=True)
            most = count if most is None else jnp.maximum(most, count)
        spare = ids_ref.shape[2] - ny * cap
        pieces.append(jnp.broadcast_to(most, (plane, spare)))
        named = jnp.concatenate(pieces, axis=1).astype(jnp.int32)
        ids_out[...] = named.reshape(ids_out.shape)

    with jax.named_scope("users"):
        for r in range(1, nx // 2 + 1):
            x_forward(r)
            if r == 1:
                z_forward(1)
                for step in range(1, ny):
                    arrived(pairs_all.at[y_at(-step)], i_recv.at[step])
                name_slots()
        from_partner()

    def first_pass(chunk):
        own = items_all[chunk]
        items_turned[:, block_rows(chunk)] = own.T

        for k in range(peers):
            s = contract(own, users[k * size : (k + 1) * size, :], (1, 1))
            top = jnp.max(s, axis=0, keepdims=True)
            p = jnp.exp(s - top)
            probs[chunk * peers + k] = p
            peaks[chunk, k : k + 1, :] = top
            sums[chunk, k : k + 1, :] = jnp.sum(p, axis=0, keepdims=True)

    with jax.named_scope("first"):
        first_pass(z)

        @pl.loop(1, plane)
        def _(step):
            where, there = far(step)
            send_plainly(ids_out.at[there], ids_ref.at[here], n_send.at[step], n_recv.at[step], where)

        ids_ref[here] = ids_out[here]
        for r in range(1, nz // 2 + 1):
            if r > 1:
                z_forward(r)
            if r < nz // 2:
                @pl.loop(0, 2)
                def _(side):
                    first_pass(lax.rem(z + nz + r - 2 * r * side, nz))
            else:
                first_pass(z_at(r))

    with jax.named_scope("lse"):
        tops = peaks[...]
        top = jnp.max(tops, axis=0)
        lses[me] = top + jnp.log(jnp.sum(sums[...] * jnp.exp(tops - top[None]), axis=0))
        for step in range(1, peers):
            send(lses.at[me], lses.at[me], l_send.at[step], l_recv.at[step], peer(step))
        for step in range(1, peers):
            arrived(meta_all.at[from_peer(step)], m_recv.at[step])
        for step in range(1, peers):
            arrived(lses.at[from_peer(step)], l_recv.at[step])
        parts = lses[...]
        top = jnp.max(parts, axis=0)
        total = top + jnp.log(jnp.sum(jnp.exp(parts - top[None]), axis=0))
        scale[...] = jnp.exp(tops - total[None])

    lines = lax.broadcasted_iota(jnp.int32, (size, size), 0)

    def second_pass(chunk):
        first = ((chunk * nx + x) * nc + c) * size

        for k in range(peers):
            weight = meta_all[k, 0:1, :]
            target = meta_all[k, 1:2, :].astype(jnp.int32) - first
            t = probs[chunk * peers + k] * (scale[chunk, k : k + 1, :] * weight)
            t = jnp.where(lines == target, t - weight, t)
            ds[block_rows(chunk), k * size : (k + 1) * size] = t.astype(BF16)

        gi_part[chunk] = jnp.dot(ds[block_rows(chunk), :], users[...], preferred_element_type=F32)

    def z_reduce(r, parts_of=((0, 0), (0, 1), (1, 0), (1, 1))):
        for way, half in parts_of:
            sign = signs[way]
            length = chain_length(nz, way, half)
            rows = pl.ds(half * half_size, half_size)
            dest = z_at(sign * (length - r))
            if 1 <= r <= length:
                land = z_land.at[way, half, r - 1]
                arrived(land, zr_recv.at[way, half, r - 1])
                if r < length:
                    land[...] += gi_part[dest, rows]
            if r < length:
                src = gi_part.at[dest, rows] if r == 0 else z_land.at[way, half, r - 1]
                send(src, z_land.at[way, half, r], zr_send.at[way, half, r],
                     zr_recv.at[way, half, r], {"rows_0": z_at(sign)})

    with jax.named_scope("second"):
        second_pass(z_at(nz // 2))
        z_reduce(0, ((0, 0), (1, 1)))
        second_pass(z_at(nz // 2 - 1))
        z_reduce(0, ((0, 1),))
        second_pass(z_at(1 - nz // 2))
        z_reduce(0, ((1, 0),))
        left = 2 * (nz // 2 - 2) + 1

        @pl.loop(0, left)
        def _(i):
            second_pass(lax.rem(z + nz + ((left - i) // 2) * (1 - 2 * lax.rem(i, 2)), nz))

    def user_pass(k):
        gu_part[k] = jnp.dot(items_turned[...], ds[:, block_rows(k)], preferred_element_type=F32)

    with jax.named_scope("zr1"):
        z_reduce(1)
    with jax.named_scope("userpass"):
        for step in range(nx):
            k = x_at(step) * nc + 1 - c
            user_pass(k)
            send(gu_part.at[k], gu_pair.at[x_at(step)], d_send.at[step], d_recv.at[step], partner)
        for step in range(nx):
            user_pass(x_at(step) * nc + c)
        for step in range(nx):
            arrived(gu_pair.at[x_at(step)], d_recv.at[step])
            gu_pair[x_at(step)] += gu_part[x_at(step) * nc + c]

    def x_reduce(r):
        for way, sign in enumerate(signs):
            for half in (0, 1):
                length = chain_length(nx, way, half)
                rows = pl.ds(half * half_size, half_size)
                dest = x_at(sign * (length - r))
                if 1 <= r <= length:
                    land = x_land.at[way, half, r - 1]
                    arrived(land, xr_recv.at[way, half, r - 1])
                    if r < length:
                        land[...] += gu_pair[dest, rows]
                if r < length:
                    src = gu_pair.at[dest, rows] if r == 0 else x_land.at[way, half, r - 1]
                    send(src, x_land.at[way, half, r], xr_send.at[way, half, r],
                         xr_recv.at[way, half, r], {"rows_1": x_at(sign)})

    with jax.named_scope("reduce"):
        x_reduce(0)
        for r in range(1, nx // 2 + 1):
            if r + 1 <= nz // 2:
                z_reduce(r + 1)
            x_reduce(r)

        def collected(own, land, n):
            pieces = []
            for half in (0, 1):
                got = own[half * half_size : (half + 1) * half_size]
                for way in (0, 1):
                    length = chain_length(n, way, half)
                    if length:
                        got = got + land[way, half, length - 1]
                pieces.append(got)
            return jnp.concatenate(pieces, axis=0)

    with jax.named_scope("towerback"):
        gu = collected(gu_pair[x], x_land, nx).astype(BF16)
        pre = pre_keep[...]
        gate = jax.nn.sigmoid(pre)
        back = jnp.dot(w2_ref[...], gu, preferred_element_type=F32)
        grad_pre = (back * gate * (1.0 + pre * (1.0 - gate))).astype(BF16)
        df_keep[0] = jnp.dot(grad_pre, feat_ref[...], preferred_element_type=F32)
        df_keep[1] = jnp.dot(gu, hid_keep[...], preferred_element_type=F32)

    with jax.named_scope("zrlast"):
        send(df_keep.at[1 - c], df_pair, ac_send, ac_recv, partner)
        for r in range(nx // 2 + 2, nz // 2 + 1):
            z_reduce(r)
        gi = collected(gi_part[z], z_land, nz).astype(BF16)
    with jax.named_scope("shares"):
        for to in range(ny):
            cols = slice(to * share, (to + 1) * share)
            share_out[to] = jnp.concatenate([gi[:half_size, cols], gi[half_size:, cols]], axis=1)
        for step in range(1, ny):
            send(share_out.at[y_at(step)], share_in.at[y], s_send.at[step], s_recv.at[step],
                 {"grp": y_at(step)})
        share_in[y] = share_out[y]
    with jax.named_scope("acy"):
        arrived(df_pair, ac_recv)
        y_part[...] = (df_keep[c] + df_pair[...]).reshape(y_part.shape)
        for step in range(1, ny):
            send(y_part.at[y_at(step)], y_land.at[step - 1], ay_send.at[step], ay_recv.at[step],
                 {"grp": y_at(step)})
    with jax.named_scope("sharewait"):
        for step in range(1, ny):
            arrived(share_in.at[y_at(-step)], s_recv.at[step])
    with jax.named_scope("slots"):
        slot_lines = lax.broadcasted_iota(jnp.int32, (plane * cap, size), 0)
        for pair in range(ny // 2):
            sides = []
            for g in (2 * pair, 2 * pair + 1):
                chosen = (slot_lines == slots_keep[g]).astype(BF16)
                packed = share_in[g]
                data = jnp.concatenate([packed[:, :share], packed[:, share:]], axis=0)
                sides.append(jnp.dot(chosen, data, preferred_element_type=F32))
            both = jnp.concatenate(sides, axis=1).astype(BF16)
            slotted[:, pair] = both.reshape(plane, cap, 2 * share)

        def exchange(first, last):
            @pl.loop(first, last)
            def _(step):
                where, there = far(step)
                send_plainly(slotted.at[there], got_ref.at[here], e_send.at[step], e_recv.at[step],
                             where)

        exchange(1, plane // 4)
        got_ref[here] = slotted[here]
    with jax.named_scope("ysum"):
        whole = y_part[y]
        for step in range(1, ny):
            arrived(y_land.at[step - 1], ay_recv.at[step])
            whole = whole + y_land[step - 1]
        p_part[...] = whole.reshape(p_part.shape)

        @pl.loop(1, tiles)
        def _(step):
            where, there = far_tile(step)
            send_plainly(p_part.at[there], p_land.at[step], ap_send.at[step], ap_recv.at[step], where)

        exchange(plane // 4, plane // 2)
        p_land[0] = p_part[tile]
    with jax.named_scope("planesum"):
        @pl.loop(1, tiles)
        def _(step):
            arrived(p_land.at[step], ap_recv.at[step])

        own = tower_ref.at[c, y, tile]
        own[...] = jnp.sum(p_land[...], axis=0)

        @pl.loop(1, tiles)
        def _(step):
            where, _ = far_tile(step)
            send_plainly(own, own, gp_send.at[step], gp_recv.at[step], where)

        exchange(plane // 2, plane)
    with jax.named_scope("planeback"):

        @pl.loop(1, tiles)
        def _(step):
            arrived(tower_ref.at[c, y, from_far_tile(step)], gp_recv.at[step])

    with jax.named_scope("yback"):
        for step in range(1, ny):
            send(tower_ref.at[c, y], tower_ref.at[c, y], gy_send.at[step], gy_recv.at[step],
                 {"grp": y_at(step)})
        for step in range(1, ny):
            arrived(tower_ref.at[c, y_at(-step)], gy_recv.at[step])
        send(tower_ref.at[c], tower_ref.at[c], gc_send, gc_recv, partner)

    with jax.named_scope("got"):
        @pl.loop(1, plane)
        def _(step):
            arrived(ids_ref.at[from_far(step)], n_recv.at[step])
            arrived(got_ref.at[from_far(step)], e_recv.at[step])

    with jax.named_scope("cback"):
        arrived(tower_ref.at[1 - c], gc_recv)
    with jax.named_scope("sent"):
        for copy in pending:
            copy.wait_send()

        @pl.loop(1, plane)
        def _(step):
            arrived(ids_out.at[0], n_send.at[step])
            arrived(slotted.at[0], e_send.at[step])

        @pl.loop(1, tiles)
        def _(step):
            arrived(p_part.at[0], ap_send.at[step])
            arrived(p_part.at[0], gp_send.at[step])


def block_grads(features, w_first, w_second, items, *columns):
    nz, nx, nc = (lax.axis_size(a) for a in ROWS)
    ny = lax.axis_size("grp")
    size, width = items.shape
    peers = nx * nc
    plane, tiles = nz * peers, nz * nx
    cap = max(2, 4 * size // plane)
    share = width // ny
    vmem, dma = pltpu.VMEM, pltpu.SemaphoreType.DMA
    zh, xh = nz // 2, nx // 2
    lane = ny * cap + 64
    tower = (nc, ny, tiles, width // ny // tiles, width)
    return pl.pallas_call(
        functools.partial(block_kernel, nz, nx, nc, ny),
        out_shape=(
            jax.ShapeDtypeStruct((plane, ny // 2, cap, 2 * share), BF16),
            jax.ShapeDtypeStruct((plane, 1, lane), jnp.int32),
            jax.ShapeDtypeStruct(tower, F32),
        ),
        in_specs=[pl.BlockSpec(memory_space=vmem)] * 8,
        out_specs=[pl.BlockSpec(memory_space=vmem)] * 3,
        scratch_shapes=[
            vmem((peers * size, width), BF16),
            vmem((nz, size, width), BF16),
            vmem((width, nz * size), BF16),
            vmem((peers, 2, size), F32),
            vmem((nz, peers, size), F32),
            vmem((nz, peers, size), F32),
            vmem((peers, peers, size), F32),
            vmem((nz, peers, size), F32),
            vmem((nz * peers, size, size), F32),
            vmem((nz * size, peers * size), BF16),
            vmem((nz, size, width), F32),
            vmem((peers, width, size), F32),
            vmem((nx, width, size), F32),
            vmem((2, 2, zh, size // 2, width), F32),
            vmem((2, 2, xh, width // 2, size), F32),
            vmem((width, size), F32),
            vmem((size, width), BF16),
            dma((2, 2, zh)), dma((2, 2, zh)),
            dma((2, 2, xh)), dma((2, 2, xh)),
            dma((2, 2, xh + 1)), dma((2, 2, xh + 1)),
            dma((peers,)), dma((peers,)),
            dma((peers,)), dma((peers,)),
            dma((2, 2, zh)), dma((2, 2, zh)),
            dma((nx,)), dma((nx,)),
            dma((2, 2, xh)), dma((2, 2, xh)),
            vmem((ny, 2, size), F32),
            vmem((ny, 1, size), jnp.int32),
            vmem((plane, 1, lane), jnp.int32),
            vmem((ny, size // 2, 2 * share), BF16),
            vmem((ny, size // 2, 2 * share), BF16),
            vmem((plane, ny // 2, cap, 2 * share), BF16),
            vmem((2, width, width), F32),
            vmem((width, width), F32),
            vmem((ny, width // ny, width), F32),
            vmem((ny - 1, width // ny, width), F32),
            vmem(tower[2:], F32),
            vmem(tower[2:], F32),
            dma((ny,)), dma((ny,)),
            dma((plane,)), dma((plane,)),
            dma((ny,)), dma((ny,)),
            dma((plane,)), dma((plane,)),
            dma, dma,
            dma((ny,)), dma((ny,)),
            dma((tiles,)), dma((tiles,)),
            dma((tiles,)), dma((tiles,)),
            dma((ny,)), dma((ny,)),
            dma, dma,
        ],
        compiler_params=pltpu.CompilerParams(
            collective_id=0, has_side_effects=True, vmem_limit_bytes=60 * 2**20
        ),
        cost_estimate=pl.CostEstimate(flops=7 * 10**9, bytes_accessed=2**20, transcendentals=2**22),
        name="block_grads",
    )(features, w_first, w_second, items, *columns)


def table_kernel(ids_ref, got_ref, tower_ref, out_ref, first_ref, second_ref, lines, *tables):
    sources, pairs, cap, lanes = got_ref.shape
    share = lanes // 2
    width = first_ref.shape[0]
    count = out_ref.shape[1]
    step = 4
    lines[...] = got_ref[...].astype(F32).reshape(lines.shape)
    for table in tables:
        table[...] = jnp.zeros_like(table)

    @pl.loop(0, sources)
    def _(source):
        @pl.loop(0, (ids_ref[source, 2 * pairs * cap] + (step - 1)) // step)
        def _(block):
            for slot in range(step):
                slot = block * step + slot
                for pair in range(pairs):
                    line = lines[pl.ds((source * pairs + pair) * cap + slot, 1), :]
                    for side in (0, 1):
                        g = 2 * pair + side
                        at = pl.ds(ids_ref[source, g * cap + slot], 1)
                        tables[g][at, :] += line

    part = min(count, 512)
    for at in range(0, count, part):
        rows = slice(at, at + part)
        even = sum(t[rows, :] for t in tables[0::2])
        odd = sum(t[rows, :] for t in tables[1::2])
        out_ref[:, rows] = even.T[:share, :] + odd.T[share:, :]
    first_ref[...] = tower_ref[0].reshape(width, width).T
    second_ref[...] = tower_ref[1].reshape(width, width).T


def table_grads(ids, got, tower):
    sources, pairs, cap, lanes = got.shape
    width = tower.shape[-1]
    vmem = pltpu.VMEM
    return pl.pallas_call(
        table_kernel,
        out_shape=(
            jax.ShapeDtypeStruct((lanes // 2, ITEMS_DEV), F32),
            jax.ShapeDtypeStruct((width, width), F32),
            jax.ShapeDtypeStruct((width, width), F32),
        ),
        in_specs=[pl.BlockSpec(memory_space=pltpu.SMEM)] + [pl.BlockSpec(memory_space=vmem)] * 2,
        out_specs=[pl.BlockSpec(memory_space=vmem)] * 3,
        scratch_shapes=[vmem((sources * pairs * cap, lanes), F32)]
        + [vmem((ITEMS_DEV + 8, lanes), F32)] * (2 * pairs),
        compiler_params=pltpu.CompilerParams(vmem_limit_bytes=40 * 2**20),
        name="table_grads",
    )(ids, got, tower)


def body(
    user_features, w_first, w_second, item_embed, example_weight, positive, item_owner, item_row
):
    got, ids, tower = block_grads(
        user_features[0], w_first, w_second, item_embed[0],
        example_weight, positive, item_owner.reshape(positive.shape), item_row,
    )
    table, first, second = table_grads(ids.reshape(ids.shape[0], -1), got, tower)
    return (first, second, table.T)


def solution(mesh):
    torus = Mesh(
        mesh.devices.reshape(8, 4, 2, mesh.shape["grp"]), ("rows_0", "rows_1", "rows_2", "grp")
    )
    placed = (
        P("grp", ROWS, None),
        P(),
        P(),
        P("grp", ROWS, None),
        P("grp", ROWS),
        P("grp", ROWS),
        P("grp", ROWS, None),
        P("grp", ROWS),
    )
    return jax.shard_map(
        body, mesh=torus, in_specs=placed, out_specs=(P(), P(), P(ROWS, "grp")), check_vma=False
    )
```

```python
import functools
import jax
import jax.numpy as jnp
from jax import lax
from jax.experimental import pallas as pl
from jax.experimental.pallas import tpu as pltpu
from jax.sharding import Mesh
from jax.sharding import PartitionSpec as P

ITEMS_DEV = 4096
HIGH = 256
ROWS = ("rows_0", "rows_1", "rows_2")
MESH = pl.DeviceIdType.MESH
F32 = jnp.float32
BF16 = jnp.bfloat16


def chain_length(n, way, half):
    return n // 2 if (way == 0) == (half == 0) else n // 2 - 1


def contract(left, right, dims):
    return lax.dot_general(left, right, ((dims[:1], dims[1:]), ((), ())), preferred_element_type=F32)


def block_kernel(
    nz, nx, nc, ny, feat_ref, w1_ref, w2_ref, items_ref, weight_ref, target_ref, owner_ref, row_ref,
    table_ref, first_ref, second_ref,
    users, items_all, items_turned, meta_all, peaks, sums, lses, scale, probs, ds,
    gi_part, gu_part, gu_pair, z_land, x_land, pre_keep, hid_keep,
    z_send, z_recv, x_send, x_recv, p_send, p_recv, m_send, m_recv, l_send, l_recv,
    zr_send, zr_recv, d_send, d_recv, xr_send, xr_recv,
    pairs_all, slots_keep, ids_out, share_out, share_in, slotted,
    df_keep, df_pair, y_part, y_land, p_part, p_land,
    i_send, i_recv, n_send, n_recv, s_send, s_recv, e_send, e_recv,
    ac_send, ac_recv, ay_send, ay_recv, ap_send, ap_recv,
    gp_send, gp_recv, gy_send, gy_recv, gc_send, gc_recv,
    landed, ids_land, tower, low_all, high_all, spread_left, spread_right, acc,
):
    z, x, c = lax.axis_index("rows_0"), lax.axis_index("rows_1"), lax.axis_index("rows_2")
    y = lax.axis_index("grp")
    size = items_ref.shape[0]
    half_size = size // 2
    peers = nx * nc
    me = x * nc + c
    signs = (1, -1)
    early, late = ((0, 0), (1, 1)), ((0, 1), (1, 0))

    def z_at(step):
        return lax.rem(z + step + nz, nz)

    def x_at(step):
        return lax.rem(x + step + nx, nx)

    def peer(step):
        dx, dc = divmod(step, nc)
        return {"rows_1": x_at(dx), "rows_2": lax.rem(c + dc, nc)}

    def from_peer(step):
        dx, dc = divmod(step, nc)
        return x_at(-dx) * nc + lax.rem(c + nc - dc, nc)

    partner = {"rows_2": 1 - c}
    pending = []

    def send(src, dst, send_sem, recv_sem, where):
        copy = pltpu.make_async_remote_copy(
            src_ref=src, dst_ref=dst, send_sem=send_sem, recv_sem=recv_sem,
            device_id=where, device_id_type=MESH,
        )
        copy.start()
        pending.append(copy)

    def arrived(ref, recv_sem):
        pltpu.make_async_copy(ref, ref, recv_sem).wait()

    barrier = pltpu.get_barrier_semaphore()
    plane = nz * peers
    here = z * peers + me
    tiles = nz * nx
    tile = z * nx + x

    def far(step):
        to_z = lax.rem(z + step // peers, nz)
        to_x = lax.rem(x + (step % peers) // nc, nx)
        to_c = lax.rem(c + step % nc, nc)
        return {"rows_0": to_z, "rows_1": to_x, "rows_2": to_c}, (to_z * nx + to_x) * nc + to_c

    def from_far(step):
        of_z = lax.rem(z + nz - step // peers, nz)
        of_x = lax.rem(x + nx - (step % peers) // nc, nx)
        of_c = lax.rem(c + nc - step % nc, nc)
        return (of_z * nx + of_x) * nc + of_c

    def far_tile(step):
        to_z, to_x = lax.rem(z + step // nx, nz), lax.rem(x + step % nx, nx)
        return {"rows_0": to_z, "rows_1": to_x}, to_z * nx + to_x

    def from_far_tile(step):
        return lax.rem(z + nz - step // nx, nz) * nx + lax.rem(x + nx - step % nx, nx)

    def y_at(step):
        return lax.rem(y + step + ny, ny)

    def send_plainly(src, dst, send_sem, recv_sem, where):
        pltpu.make_async_remote_copy(
            src_ref=src, dst_ref=dst, send_sem=send_sem, recv_sem=recv_sem,
            device_id=where, device_id_type=MESH,
        ).start()

    @pl.loop(1, plane)
    def _(step):
        pl.semaphore_signal(barrier, inc=1, device_id=far(step)[0], device_id_type=MESH)

    for step in range(1, ny):
        pl.semaphore_signal(barrier, inc=1, device_id={"grp": y_at(step)}, device_id_type=MESH)

    def rows_of(block, half):
        return pl.ds(pl.multiple_of(block * size + half * half_size, half_size), half_size)

    def block_rows(block):
        return pl.ds(pl.multiple_of(block * size, size), size)

    with jax.named_scope("tower"):
        pre = jnp.dot(feat_ref[...], w1_ref[...], preferred_element_type=F32)
        hidden = (pre * jax.nn.sigmoid(pre)).astype(BF16)
        hid_keep[...] = hidden
        users[block_rows(me), :] = jnp.dot(hidden, w2_ref[...], preferred_element_type=F32).astype(BF16)
        items_all[z] = items_ref[...]
        meta_all[me, 0:1, :] = weight_ref[...]
        meta_all[me, 1:2, :] = target_ref[...].astype(F32)

        pairs_all[y, 0:1, :] = owner_ref[...].astype(F32)
        pairs_all[y, 1:2, :] = row_ref[...].astype(F32)
    with jax.named_scope("barrier"):
        pl.semaphore_wait(barrier, plane - 1 + ny - 1)

    def z_forward(r, parts_of):
        for way, half in parts_of:
            sign = signs[way]
            length = chain_length(nz, way, half)
            rows = pl.ds(half * half_size, half_size)
            block = z_at(-sign * r)
            if 1 <= r <= length:
                arrived(items_all.at[block, rows], z_recv.at[way, half, r - 1])
            if r < length:
                src = items_ref.at[rows] if r == 0 else items_all.at[block, rows]
                send(src, items_all.at[block, rows], z_send.at[way, half, r],
                     z_recv.at[way, half, r], {"rows_0": z_at(sign)})

    def x_forward(r, parts_of):
        for way, half in parts_of:
            sign = signs[way]
            length = chain_length(nx, way, half)
            place = users.at[rows_of(x_at(-sign * r) * nc + c, half)]
            if 1 <= r <= length:
                arrived(place, x_recv.at[way, half, r - 1])
            if r < length:
                send(place, place, x_send.at[way, half, r], x_recv.at[way, half, r],
                     {"rows_1": x_at(sign)})
            if 1 <= r <= length:
                send(place, place, p_send.at[way, half, r], p_recv.at[way, half, r], partner)
            if r == 0 and way == 0:
                send(place, place, p_send.at[way, half, 0], p_recv.at[way, half, 0], partner)

    def from_partner():
        for way, sign in enumerate(signs):
            for half in (0, 1):
                for r in range(1 if way else 0, chain_length(nx, way, half) + 1):
                    place = users.at[rows_of(x_at(-sign * r) * nc + 1 - c, half)]
                    arrived(place, p_recv.at[way, half, r])

    with jax.named_scope("start"):
        for parts in (early, late):
            x_forward(0, parts)
            z_forward(0, parts)
        for step in range(1, peers):
            send(meta_all.at[me], meta_all.at[me], m_send.at[step], m_recv.at[step], peer(step))

        for step in range(1, ny):
            send(pairs_all.at[y], pairs_all.at[y], i_send.at[step], i_recv.at[step],
                 {"grp": y_at(step)})

        pre_keep[...] = pre.T

    cap = landed.shape[2]
    share = landed.shape[3] // 2

    def name_slots():
        earlier = (
            lax.broadcasted_iota(jnp.int32, (size, size), 0)
            < lax.broadcasted_iota(jnp.int32, (size, size), 1)
        ).astype(BF16)
        owner_lines = lax.broadcasted_iota(jnp.int32, (plane, size), 0)
        rank_lines = lax.broadcasted_iota(jnp.int32, (cap, size), 0)
        pieces = []
        for g in range(ny):
            owner = pairs_all[g, 0:1, :].astype(jnp.int32)
            row = pairs_all[g, 1:2, :]
            member = (owner_lines == owner).astype(F32)
            before = jnp.dot(member.astype(BF16), earlier, preferred_element_type=F32)
            rank = jnp.sum(before * member, axis=0, keepdims=True).astype(jnp.int32)
            slots_keep[g] = owner * cap + rank
            at_rank = (rank_lines == rank).astype(BF16)
            high = jnp.floor(row * (1.0 / 64.0))
            low = row - 64.0 * high
            found = contract(member.astype(BF16), at_rank, (1, 1))
            ids = 64.0 * contract((member * high).astype(BF16), at_rank, (1, 1)) + contract(
                (member * low).astype(BF16), at_rank, (1, 1)
            )
            pieces.append(jnp.where(found > 0.5, ids, float(ITEMS_DEV)))
        spare = ids_out.shape[2] - ny * cap
        pieces.append(jnp.zeros((plane, spare), F32))
        named = jnp.concatenate(pieces, axis=1).astype(jnp.int32)
        ids_out[...] = named.reshape(ids_out.shape)

    with jax.named_scope("users"):
        for r in (1, 2):
            for parts in (early, late):
                if r < nz // 2 or parts is early:
                    z_forward(r, parts)
                if r <= nx // 2:
                    x_forward(r, parts)
        from_partner()

    def first_pass(chunk):
        own = items_all[chunk]
        items_turned[:, block_rows(chunk)] = own.T

        for k in range(peers):
            s = contract(own, users[k * size : (k + 1) * size, :], (1, 1))
            top = jnp.max(s, axis=0, keepdims=True)
            p = jnp.exp(s - top)
            probs[chunk * peers + k] = p
            peaks[chunk, k : k + 1, :] = top
            sums[chunk, k : k + 1, :] = jnp.sum(p, axis=0, keepdims=True)

    batch, batches = peers, nz
    high_span = acc.shape[1]
    low_count = acc.shape[0] // share

    def read_slots():
        @pl.loop(1, plane)
        def _(step):
            arrived(ids_land.at[from_far(step)], n_recv.at[step])
            arrived(ids_out.at[0], n_send.at[step])

        rows = ids_land[...].reshape(plane, ids_land.shape[2]).astype(F32)
        low = jnp.floor(rows * (1.0 / high_span))
        high = rows - high_span * low
        lanes = (ids_land.shape[2], batch * cap)
        slot_of = lax.broadcasted_iota(jnp.int32, lanes, 0)
        place_of = lax.rem(lax.broadcasted_iota(jnp.int32, lanes, 1), cap)
        at = (plane, batch * cap)
        mine = lax.rem(lax.broadcasted_iota(jnp.int32, at, 0), batch) == (
            lax.broadcasted_iota(jnp.int32, at, 1) // cap
        )
        for g in range(ny):
            spread = (slot_of == place_of + g * cap).astype(BF16)
            for part, keep in ((low, low_all), (high, high_all)):
                wide = jnp.dot(part.astype(BF16), spread, preferred_element_type=F32)
                wide = jnp.where(mine, wide, 0.0).reshape(batches, batch, batch * cap)
                keep[g] = jnp.sum(wide, axis=1).astype(jnp.int32)

    with jax.named_scope("first"):
        first_pass(z)
        for r in range(1, nz // 2):
            if 2 < r + 1 < nz // 2:
                z_forward(r + 1, early)

            @pl.loop(0, 2)
            def _(side):
                first_pass(lax.rem(z + nz + r - 2 * r * side, nz))

            if 2 < r + 1:
                z_forward(r + 1, late if r + 1 < nz // 2 else early)
        first_pass(z_at(nz // 2))
    with jax.named_scope("lse"):
        tops = peaks[...]
        top = jnp.max(tops, axis=0)
        lses[me] = top + jnp.log(jnp.sum(sums[...] * jnp.exp(tops - top[None]), axis=0))
        for step in range(1, peers):
            send(lses.at[me], lses.at[me], l_send.at[step], l_recv.at[step], peer(step))
        for step in range(1, peers):
            arrived(meta_all.at[from_peer(step)], m_recv.at[step])
        for step in range(1, peers):
            arrived(lses.at[from_peer(step)], l_recv.at[step])
        parts = lses[...]
        top = jnp.max(parts, axis=0)
        total = top + jnp.log(jnp.sum(jnp.exp(parts - top[None]), axis=0))
        scale[...] = jnp.exp(tops - total[None])

    lines = lax.broadcasted_iota(jnp.int32, (size, size), 0)

    def second_pass(chunk):
        first = ((chunk * nx + x) * nc + c) * size

        for k in range(peers):
            weight = meta_all[k, 0:1, :]
            target = meta_all[k, 1:2, :].astype(jnp.int32) - first
            t = probs[chunk * peers + k] * (scale[chunk, k : k + 1, :] * weight)
            t = jnp.where(lines == target, t - weight, t)
            ds[block_rows(chunk), k * size : (k + 1) * size] = t.astype(BF16)

        gi_part[chunk] = jnp.dot(ds[block_rows(chunk), :], users[...], preferred_element_type=F32)

    def z_reduce(r, parts_of=((0, 0), (0, 1), (1, 0), (1, 1))):
        for way, half in parts_of:
            sign = signs[way]
            length = chain_length(nz, way, half)
            rows = pl.ds(half * half_size, half_size)
            dest = z_at(sign * (length - r))
            if 1 <= r <= length:
                land = z_land.at[way, half, r - 1]
                arrived(land, zr_recv.at[way, half, r - 1])
                if r < length:
                    land[...] += gi_part[dest, rows]
            if r < length:
                src = gi_part.at[dest, rows] if r == 0 else z_land.at[way, half, r - 1]
                send(src, z_land.at[way, half, r], zr_send.at[way, half, r],
                     zr_recv.at[way, half, r], {"rows_0": z_at(sign)})

    with jax.named_scope("second"):
        second_pass(z_at(nz // 2))
        z_reduce(0, ((0, 0), (1, 1)))
        second_pass(z_at(nz // 2 - 1))
        z_reduce(0, ((0, 1),))
        second_pass(z_at(1 - nz // 2))
        z_reduce(0, ((1, 0),))
        left = 2 * (nz // 2 - 2) + 1

        @pl.loop(0, left)
        def _(i):
            second_pass(lax.rem(z + nz + ((left - i) // 2) * (1 - 2 * lax.rem(i, 2)), nz))

    def user_pass(k):
        gu_part[k] = jnp.dot(items_turned[...], ds[:, block_rows(k)], preferred_element_type=F32)

    def collected(own, land, n):
        pieces = []
        for half in (0, 1):
            got = own[half * half_size : (half + 1) * half_size]
            for way in (0, 1):
                length = chain_length(n, way, half)
                if length:
                    got = got + land[way, half, length - 1]
            pieces.append(got)
        return jnp.concatenate(pieces, axis=0)


    def x_reduce(r, parts_of):
        for way, half in parts_of:
            sign = signs[way]
            length = chain_length(nx, way, half)
            rows = pl.ds(half * half_size, half_size)
            dest = x_at(sign * (length - r))
            if 1 <= r <= length:
                land = x_land.at[way, half, r - 1]
                arrived(land, xr_recv.at[way, half, r - 1])
                if r < length:
                    land[...] += gu_pair[dest, rows]
            if r < length:
                src = gu_pair.at[dest, rows] if r == 0 else x_land.at[way, half, r - 1]
                send(src, x_land.at[way, half, r], xr_send.at[way, half, r],
                     xr_recv.at[way, half, r], {"rows_1": x_at(sign)})

    with jax.named_scope("zr1"):
        z_reduce(1, early)
    with jax.named_scope("userpass"):
        for step in range(nx):
            k = x_at(step) * nc + 1 - c
            user_pass(k)
            send(gu_part.at[k], gu_pair.at[x_at(step)], d_send.at[step], d_recv.at[step], partner)
        for step in range(nx // 2):
            user_pass(x_at(step) * nc + c)
        z_reduce(1, late)
        for step in range(nx // 2, nx):
            user_pass(x_at(step) * nc + c)
        for step in range(nx):
            arrived(gu_pair.at[x_at(step)], d_recv.at[step])
            gu_pair[x_at(step)] += gu_part[x_at(step) * nc + c]
    with jax.named_scope("reduce"):
        x_reduce(0, early)
        x_reduce(0, late)
        for step in range(1, ny):
            arrived(pairs_all.at[y_at(-step)], i_recv.at[step])
        name_slots()

        @pl.loop(1, plane)
        def _(step):
            where, there = far(step)
            send_plainly(ids_out.at[there], ids_land.at[here], n_send.at[step], n_recv.at[step], where)

        ids_land[here] = ids_out[here]
        along_z = [(r, parts) for r in range(2, nz // 2) for parts in (early, late)]
        along_x = [(r, parts) for r in range(1, nx // 2 + 1) for parts in (early, late)]
        for event in along_z[:2]:
            z_reduce(*event)
        along_z = along_z[2:]
        while along_z or along_x:
            if along_x:
                x_reduce(*along_x.pop(0))
            if along_z:
                z_reduce(*along_z.pop(0))
    with jax.named_scope("towerback"):
        gu = collected(gu_pair[x], x_land, nx).astype(BF16)
        pre = pre_keep[...]
        gate = jax.nn.sigmoid(pre)
        back = jnp.dot(w2_ref[...], gu, preferred_element_type=F32)
        grad_pre = (back * gate * (1.0 + pre * (1.0 - gate))).astype(BF16)
        df_keep[0] = jnp.dot(grad_pre, feat_ref[...], preferred_element_type=F32)
        df_keep[1] = jnp.dot(gu, hid_keep[...], preferred_element_type=F32)

    with jax.named_scope("zrlast"):
        send(df_keep.at[1 - c], df_pair, ac_send, ac_recv, partner)
        z_reduce(nz // 2, early)
        gi = collected(gi_part[z], z_land, nz).astype(BF16)
    with jax.named_scope("shares"):
        for to in range(ny):
            cols = slice(to * share, (to + 1) * share)
            share_out[to] = jnp.concatenate([gi[:half_size, cols], gi[half_size:, cols]], axis=1)
        for step in range(1, ny):
            send(share_out.at[y_at(step)], share_in.at[y], s_send.at[step], s_recv.at[step],
                 {"grp": y_at(step)})
        share_in[y] = share_out[y]
    with jax.named_scope("acy"):
        arrived(df_pair, ac_recv)
        y_part[...] = (df_keep[c] + df_pair[...]).reshape(y_part.shape)
        for step in range(1, ny):
            send(y_part.at[y_at(step)], y_land.at[step - 1], ay_send.at[step], ay_recv.at[step],
                 {"grp": y_at(step)})
    with jax.named_scope("readslots"):
        read_slots()
    with jax.named_scope("sharewait"):
        for step in range(1, ny):
            arrived(share_in.at[y_at(-step)], s_recv.at[step])
    with jax.named_scope("slots"):
        slot_lines = lax.broadcasted_iota(jnp.int32, (plane * cap, size), 0)
        for pair in range(ny // 2):
            sides = []
            for g in (2 * pair, 2 * pair + 1):
                chosen = (slot_lines == slots_keep[g]).astype(BF16)
                packed = share_in[g]
                data = jnp.concatenate([packed[:, :share], packed[:, share:]], axis=0)
                sides.append(jnp.dot(chosen, data, preferred_element_type=F32))
            both = jnp.concatenate(sides, axis=1).astype(BF16)
            slotted[:, pair] = both.reshape(plane, cap, 2 * share)

        def exchange(first, last):
            @pl.loop(first, last)
            def _(turn):
                pick, odd = turn // peers // 2, lax.rem(turn // peers, 2)
                dz = (1 - odd) * (nz // 2 + pick) + odd * (nz // 2 - 1 - pick)
                step = dz * peers + peers - 1 - lax.rem(turn, peers)
                where, there = far(step)
                send_plainly(slotted.at[there], landed.at[here], e_send.at[step], e_recv.at[step],
                             where)

        landed[here] = slotted[here]
        acc[...] = jnp.zeros_like(acc)
    with jax.named_scope("ysum"):
        whole = y_part[y]
        for step in range(1, ny):
            arrived(y_land.at[step - 1], ay_recv.at[step])
            whole = whole + y_land[step - 1]
        p_part[...] = whole.reshape(p_part.shape)

        @pl.loop(1, tiles)
        def _(step):
            where, there = far_tile(step)
            send_plainly(p_part.at[there], p_land.at[step], ap_send.at[step], ap_recv.at[step], where)

        exchange(0, plane // 4)
        p_land[0] = p_part[tile]
    with jax.named_scope("planesum"):
        @pl.loop(1, tiles)
        def _(step):
            arrived(p_land.at[step], ap_recv.at[step])
            arrived(p_part.at[0], ap_send.at[step])

        own = tower.at[c, y, tile]
        own[...] = jnp.sum(p_land[...], axis=0)

        @pl.loop(1, tiles)
        def _(step):
            where, _ = far_tile(step)
            send_plainly(own, own, gp_send.at[step], gp_recv.at[step], where)

        exchange(plane // 4, plane - 1)
    long = batch * cap

    def add_rows(b):
        for unit, dz in enumerate((nz // 2 + b, nz // 2 - 1 - b)):
            @pl.loop(0 if dz else 1, peers)
            def _(inner):
                arrived(landed.at[from_far(dz * peers + inner)], e_recv.at[dz * peers + inner])
                arrived(slotted.at[0], e_send.at[dz * peers + inner])

            source = z_at(-dz)
            for pair in range(ny // 2):
                block = landed[pl.ds(source * batch, batch), pair].reshape(long, 2 * share)
                turned = block.T
                for side in (0, 1):
                    g = 2 * pair + side
                    data = turned[side * share : (side + 1) * share, :]
                    low = low_all[g, pl.ds(source, 1), :]
                    cols = slice((2 * g + unit) * long, (2 * g + unit + 1) * long)
                    for at in range(low_count):
                        spread_left[at * share : (at + 1) * share, cols] = data * (
                            low == at
                        ).astype(BF16)
                    lines_of = lax.broadcasted_iota(jnp.int32, (high_span, long), 0)
                    high = high_all[g, pl.ds(source, 1), :]
                    spread_right[:, cols] = (lines_of == high).astype(BF16)
        acc[...] += contract(spread_left[...], spread_right[...], (1, 1))

    with jax.named_scope("add0"):
        add_rows(0)
    with jax.named_scope("planeback"):
        @pl.loop(1, tiles)
        def _(step):
            arrived(tower.at[c, y, from_far_tile(step)], gp_recv.at[step])
            arrived(p_part.at[0], gp_send.at[step])

        for step in range(1, ny):
            send(tower.at[c, y], tower.at[c, y], gy_send.at[step], gy_recv.at[step],
                 {"grp": y_at(step)})
    with jax.named_scope("add1"):
        for b in range(1, nz // 2 - 1):
            add_rows(b)
    with jax.named_scope("yback"):
        for step in range(1, ny):
            arrived(tower.at[c, y_at(-step)], gy_recv.at[step])
        send(tower.at[c], tower.at[c], gc_send, gc_recv, partner)
    with jax.named_scope("add3"):
        add_rows(nz // 2 - 1)
        for at in range(low_count):
            table_ref[:, at * high_span : (at + 1) * high_span] = acc[at * share : (at + 1) * share, :]
    with jax.named_scope("cback"):
        arrived(tower.at[1 - c], gc_recv)
        width = first_ref.shape[0]
        first_ref[...] = tower[0].reshape(width, width).T
        second_ref[...] = tower[1].reshape(width, width).T
    with jax.named_scope("sent"):
        for copy in pending:
            copy.wait_send()


def block_grads(features, w_first, w_second, items, *columns):
    nz, nx, nc = (lax.axis_size(a) for a in ROWS)
    ny = lax.axis_size("grp")
    size, width = items.shape
    peers = nx * nc
    plane, tiles = nz * peers, nz * nx
    cap = max(2, 4 * size // plane)
    share = width // ny
    vmem, dma = pltpu.VMEM, pltpu.SemaphoreType.DMA
    zh, xh = nz // 2, nx // 2
    lane = ny * cap + 64
    tower = (nc, ny, tiles, width // ny // tiles, width)
    return pl.pallas_call(
        functools.partial(block_kernel, nz, nx, nc, ny),
        out_shape=(
            jax.ShapeDtypeStruct((share, ITEMS_DEV), F32),
            jax.ShapeDtypeStruct((width, width), F32),
            jax.ShapeDtypeStruct((width, width), F32),
        ),
        in_specs=[pl.BlockSpec(memory_space=vmem)] * 8,
        out_specs=[pl.BlockSpec(memory_space=vmem)] * 3,
        scratch_shapes=[
            vmem((peers * size, width), BF16),
            vmem((nz, size, width), BF16),
            vmem((width, nz * size), BF16),
            vmem((peers, 2, size), F32),
            vmem((nz, peers, size), F32),
            vmem((nz, peers, size), F32),
            vmem((peers, peers, size), F32),
            vmem((nz, peers, size), F32),
            vmem((nz * peers, size, size), F32),
            vmem((nz * size, peers * size), BF16),
            vmem((nz, size, width), F32),
            vmem((peers, width, size), F32),
            vmem((nx, width, size), F32),
            vmem((2, 2, zh, size // 2, width), F32),
            vmem((2, 2, xh, width // 2, size), F32),
            vmem((width, size), F32),
            vmem((size, width), BF16),
            dma((2, 2, zh)), dma((2, 2, zh)),
            dma((2, 2, xh)), dma((2, 2, xh)),
            dma((2, 2, xh + 1)), dma((2, 2, xh + 1)),
            dma((peers,)), dma((peers,)),
            dma((peers,)), dma((peers,)),
            dma((2, 2, zh)), dma((2, 2, zh)),
            dma((nx,)), dma((nx,)),
            dma((2, 2, xh)), dma((2, 2, xh)),
            vmem((ny, 2, size), F32),
            vmem((ny, 1, size), jnp.int32),
            vmem((plane, 1, lane), jnp.int32),
            vmem((ny, size // 2, 2 * share), BF16),
            vmem((ny, size // 2, 2 * share), BF16),
            vmem((plane, ny // 2, cap, 2 * share), BF16),
            vmem((2, width, width), F32),
            vmem((width, width), F32),
            vmem((ny, width // ny, width), F32),
            vmem((ny - 1, width // ny, width), F32),
            vmem(tower[2:], F32),
            vmem(tower[2:], F32),
            dma((ny,)), dma((ny,)),
            dma((plane,)), dma((plane,)),
            dma((ny,)), dma((ny,)),
            dma((plane,)), dma((plane,)),
            dma, dma,
            dma((ny,)), dma((ny,)),
            dma((tiles,)), dma((tiles,)),
            dma((tiles,)), dma((tiles,)),
            dma((ny,)), dma((ny,)),
            dma, dma,
            vmem((plane, ny // 2, cap, 2 * share), BF16),
            vmem((plane, 1, lane), jnp.int32),
            vmem(tower, F32),
            vmem((ny, nz, peers * cap), jnp.int32),
            vmem((ny, nz, peers * cap), jnp.int32),
            vmem((ITEMS_DEV // HIGH * share, ny * 2 * peers * cap), BF16),
            vmem((HIGH, ny * 2 * peers * cap), BF16),
            vmem((ITEMS_DEV // HIGH * share, HIGH), F32),
        ],
        compiler_params=pltpu.CompilerParams(
            collective_id=0, has_side_effects=True, vmem_limit_bytes=60 * 2**20
        ),
        cost_estimate=pl.CostEstimate(flops=7 * 10**9, bytes_accessed=2**20, transcendentals=2**22),
        name="block_grads",
    )(features, w_first, w_second, items, *columns)


def finish_kernel(*refs):
    count = (len(refs) - 1) // 2
    copies = [
        pltpu.make_async_copy(refs[i], refs[count + i], refs[-1].at[i]) for i in range(count)
    ]
    for copy in copies:
        copy.start()
    for copy in copies:
        copy.wait()


def finish(*arrays):
    return pl.pallas_call(
        finish_kernel,
        out_shape=tuple(jax.ShapeDtypeStruct(a.shape, a.dtype) for a in arrays),
        in_specs=[pl.BlockSpec(memory_space=pl.ANY)] * len(arrays),
        out_specs=[pl.BlockSpec(memory_space=pltpu.VMEM)] * len(arrays),
        scratch_shapes=[pltpu.SemaphoreType.DMA((len(arrays),))],
        name="finish",
    )(*arrays)


def body(
    user_features, w_first, w_second, item_embed, example_weight, positive, item_owner, item_row
):
    table, first, second = block_grads(
        user_features[0], w_first, w_second, item_embed[0],
        example_weight, positive, item_owner.reshape(positive.shape), item_row,
    )
    table, first, second = finish(table, first, second)
    return (first, second, table.T)


def solution(mesh):
    torus = Mesh(
        mesh.devices.reshape(8, 4, 2, mesh.shape["grp"]), ("rows_0", "rows_1", "rows_2", "grp")
    )
    placed = (
        P("grp", ROWS, None),
        P(),
        P(),
        P("grp", ROWS, None),
        P("grp", ROWS),
        P("grp", ROWS),
        P("grp", ROWS, None),
        P("grp", ROWS),
    )
    return jax.shard_map(
        body, mesh=torus, in_specs=placed, out_specs=(P(), P(), P(ROWS, "grp")), check_vma=False
    )
```

```python
import functools
import jax
import jax.numpy as jnp
from jax import lax
from jax.experimental import pallas as pl
from jax.experimental.pallas import tpu as pltpu
from jax.sharding import Mesh
from jax.sharding import PartitionSpec as P

ITEMS_DEV = 4096
HIGH = 256
ROWS = ("rows_0", "rows_1", "rows_2")
MESH = pl.DeviceIdType.MESH
F32 = jnp.float32
BF16 = jnp.bfloat16


def chain_length(n, way, half):
    return n // 2 if (way == 0) == (half == 0) else n // 2 - 1


def contract(left, right, dims):
    return lax.dot_general(left, right, ((dims[:1], dims[1:]), ((), ())), preferred_element_type=F32)


def block_kernel(
    nz, nx, nc, ny, feat_ref, w1_ref, w2_ref, items_ref, weight_ref, target_ref, owner_ref, row_ref,
    table_ref, first_ref, second_ref,
    users, items_all, items_turned, meta_all, peaks, sums, lses, scale, probs, ds,
    gi_part, gu_part, gu_pair, z_land, x_land, pre_keep, hid_keep,
    z_send, z_recv, x_send, x_recv, p_send, p_recv, m_send, m_recv, l_send, l_recv,
    zr_send, zr_recv, d_send, d_recv, xr_send, xr_recv,
    pairs_all, slots_keep, ids_out, share_out, share_in, slotted,
    df_keep, df_pair, y_part, y_land, p_part, p_land,
    i_send, i_recv, n_send, n_recv, s_send, s_recv, e_send, e_recv,
    ac_send, ac_recv, ay_send, ay_recv, ap_send, ap_recv,
    gp_send, gp_recv, gy_send, gy_recv, gc_send, gc_recv,
    landed, ids_land, tower, low_all, high_all, spread_left, spread_right, acc,
):
    z, x, c = lax.axis_index("rows_0"), lax.axis_index("rows_1"), lax.axis_index("rows_2")
    y = lax.axis_index("grp")
    size = items_ref.shape[0]
    half_size = size // 2
    peers = nx * nc
    me = x * nc + c
    signs = (1, -1)
    early, late = ((0, 0), (1, 1)), ((0, 1), (1, 0))

    def z_at(step):
        return lax.rem(z + step + nz, nz)

    def x_at(step):
        return lax.rem(x + step + nx, nx)

    def peer(step):
        dx, dc = divmod(step, nc)
        return {"rows_1": x_at(dx), "rows_2": lax.rem(c + dc, nc)}

    def from_peer(step):
        dx, dc = divmod(step, nc)
        return x_at(-dx) * nc + lax.rem(c + nc - dc, nc)

    partner = {"rows_2": 1 - c}
    pending = []

    def send(src, dst, send_sem, recv_sem, where):
        copy = pltpu.make_async_remote_copy(
            src_ref=src, dst_ref=dst, send_sem=send_sem, recv_sem=recv_sem,
            device_id=where, device_id_type=MESH,
        )
        copy.start()
        pending.append(copy)

    def arrived(ref, recv_sem):
        pltpu.make_async_copy(ref, ref, recv_sem).wait()

    barrier = pltpu.get_barrier_semaphore()
    plane = nz * peers
    here = z * peers + me
    tiles = nz * nx
    tile = z * nx + x

    def far(step):
        to_z = lax.rem(z + step // peers, nz)
        to_x = lax.rem(x + (step % peers) // nc, nx)
        to_c = lax.rem(c + step % nc, nc)
        return {"rows_0": to_z, "rows_1": to_x, "rows_2": to_c}, (to_z * nx + to_x) * nc + to_c

    def from_far(step):
        of_z = lax.rem(z + nz - step // peers, nz)
        of_x = lax.rem(x + nx - (step % peers) // nc, nx)
        of_c = lax.rem(c + nc - step % nc, nc)
        return (of_z * nx + of_x) * nc + of_c

    def far_tile(step):
        to_z, to_x = lax.rem(z + step // nx, nz), lax.rem(x + step % nx, nx)
        return {"rows_0": to_z, "rows_1": to_x}, to_z * nx + to_x

    def from_far_tile(step):
        return lax.rem(z + nz - step // nx, nz) * nx + lax.rem(x + nx - step % nx, nx)

    def y_at(step):
        return lax.rem(y + step + ny, ny)

    def send_plainly(src, dst, send_sem, recv_sem, where):
        pltpu.make_async_remote_copy(
            src_ref=src, dst_ref=dst, send_sem=send_sem, recv_sem=recv_sem,
            device_id=where, device_id_type=MESH,
        ).start()

    @pl.loop(1, plane)
    def _(step):
        pl.semaphore_signal(barrier, inc=1, device_id=far(step)[0], device_id_type=MESH)

    for step in range(1, ny):
        pl.semaphore_signal(barrier, inc=1, device_id={"grp": y_at(step)}, device_id_type=MESH)

    def rows_of(block, half):
        return pl.ds(pl.multiple_of(block * size + half * half_size, half_size), half_size)

    def block_rows(block):
        return pl.ds(pl.multiple_of(block * size, size), size)

    with jax.named_scope("tower"):
        pre = jnp.dot(feat_ref[...], w1_ref[...], preferred_element_type=F32)
        hidden = (pre * jax.nn.sigmoid(pre)).astype(BF16)
        hid_keep[...] = hidden
        users[block_rows(me), :] = jnp.dot(hidden, w2_ref[...], preferred_element_type=F32).astype(BF16)
        items_all[z] = items_ref[...]
        meta_all[me, 0:1, :] = weight_ref[...]
        meta_all[me, 1:2, :] = target_ref[...].astype(F32)

        pairs_all[y, 0:1, :] = owner_ref[...].astype(F32)
        pairs_all[y, 1:2, :] = row_ref[...].astype(F32)
    with jax.named_scope("barrier"):
        pl.semaphore_wait(barrier, plane - 1 + ny - 1)

    def z_forward(r, parts_of):
        for way, half in parts_of:
            sign = signs[way]
            length = chain_length(nz, way, half)
            rows = pl.ds(half * half_size, half_size)
            block = z_at(-sign * r)
            if 1 <= r <= length:
                arrived(items_all.at[block, rows], z_recv.at[way, half, r - 1])
            if r < length:
                src = items_ref.at[rows] if r == 0 else items_all.at[block, rows]
                send(src, items_all.at[block, rows], z_send.at[way, half, r],
                     z_recv.at[way, half, r], {"rows_0": z_at(sign)})

    def x_forward(r, parts_of):
        for way, half in parts_of:
            sign = signs[way]
            length = chain_length(nx, way, half)
            place = users.at[rows_of(x_at(-sign * r) * nc + c, half)]
            if 1 <= r <= length:
                arrived(place, x_recv.at[way, half, r - 1])
            if r < length:
                send(place, place, x_send.at[way, half, r], x_recv.at[way, half, r],
                     {"rows_1": x_at(sign)})
            if 1 <= r <= length:
                send(place, place, p_send.at[way, half, r], p_recv.at[way, half, r], partner)
            if r == 0 and way == 0:
                send(place, place, p_send.at[way, half, 0], p_recv.at[way, half, 0], partner)

    def from_partner():
        for way, sign in enumerate(signs):
            for half in (0, 1):
                for r in range(1 if way else 0, chain_length(nx, way, half) + 1):
                    place = users.at[rows_of(x_at(-sign * r) * nc + 1 - c, half)]
                    arrived(place, p_recv.at[way, half, r])

    with jax.named_scope("start"):
        for parts in (early, late):
            x_forward(0, parts)
            z_forward(0, parts)
        for step in range(1, peers):
            send(meta_all.at[me], meta_all.at[me], m_send.at[step], m_recv.at[step], peer(step))

        for step in range(1, ny):
            send(pairs_all.at[y], pairs_all.at[y], i_send.at[step], i_recv.at[step],
                 {"grp": y_at(step)})

        pre_keep[...] = pre.T

    cap = landed.shape[2]
    share = landed.shape[3] // 2

    def name_slots():
        earlier = (
            lax.broadcasted_iota(jnp.int32, (size, size), 0)
            < lax.broadcasted_iota(jnp.int32, (size, size), 1)
        ).astype(BF16)
        owner_lines = lax.broadcasted_iota(jnp.int32, (plane, size), 0)
        rank_lines = lax.broadcasted_iota(jnp.int32, (cap, size), 0)
        pieces = []
        for g in range(ny):
            owner = pairs_all[g, 0:1, :].astype(jnp.int32)
            row = pairs_all[g, 1:2, :]
            member = (owner_lines == owner).astype(F32)
            before = jnp.dot(member.astype(BF16), earlier, preferred_element_type=F32)
            rank = jnp.sum(before * member, axis=0, keepdims=True).astype(jnp.int32)
            slots_keep[g] = owner * cap + rank
            at_rank = (rank_lines == rank).astype(BF16)
            high = jnp.floor(row * (1.0 / 64.0))
            low = row - 64.0 * high
            found = contract(member.astype(BF16), at_rank, (1, 1))
            ids = 64.0 * contract((member * high).astype(BF16), at_rank, (1, 1)) + contract(
                (member * low).astype(BF16), at_rank, (1, 1)
            )
            pieces.append(jnp.where(found > 0.5, ids, float(ITEMS_DEV)))
        spare = ids_out.shape[2] - ny * cap
        pieces.append(jnp.zeros((plane, spare), F32))
        named = jnp.concatenate(pieces, axis=1).astype(jnp.int32)
        ids_out[...] = named.reshape(ids_out.shape)

    with jax.named_scope("users"):
        for r in (1, 2):
            for parts in (early, late):
                if r < nz // 2 or parts is early:
                    z_forward(r, parts)
                if r <= nx // 2:
                    x_forward(r, parts)
        from_partner()

    def first_pass(chunk):
        own = items_all[chunk]
        items_turned[:, block_rows(chunk)] = own.T

        for k in range(peers):
            s = contract(own, users[k * size : (k + 1) * size, :], (1, 1))
            top = jnp.max(s, axis=0, keepdims=True)
            p = jnp.exp(s - top)
            probs[chunk * peers + k] = p
            peaks[chunk, k : k + 1, :] = top
            sums[chunk, k : k + 1, :] = jnp.sum(p, axis=0, keepdims=True)

    batch, batches = peers, nz
    high_span = acc.shape[1]
    low_count = acc.shape[0] // share

    def read_slots():
        @pl.loop(1, plane)
        def _(step):
            arrived(ids_land.at[from_far(step)], n_recv.at[step])
            arrived(ids_out.at[0], n_send.at[step])

        rows = ids_land[...].reshape(plane, ids_land.shape[2]).astype(F32)
        low = jnp.floor(rows * (1.0 / high_span))
        high = rows - high_span * low
        lanes = (ids_land.shape[2], batch * cap)
        slot_of = lax.broadcasted_iota(jnp.int32, lanes, 0)
        place_of = lax.rem(lax.broadcasted_iota(jnp.int32, lanes, 1), cap)
        at = (plane, batch * cap)
        mine = lax.rem(lax.broadcasted_iota(jnp.int32, at, 0), batch) == (
            lax.broadcasted_iota(jnp.int32, at, 1) // cap
        )
        for g in range(ny):
            spread = (slot_of == place_of + g * cap).astype(BF16)
            for part, keep in ((low, low_all), (high, high_all)):
                wide = jnp.dot(part.astype(BF16), spread, preferred_element_type=F32)
                wide = jnp.where(mine, wide, 0.0).reshape(batches, batch, batch * cap)
                keep[g] = jnp.sum(wide, axis=1).astype(jnp.int32)

    with jax.named_scope("first"):
        first_pass(z)
        for r in range(1, nz // 2):
            if 2 < r + 1 < nz // 2:
                z_forward(r + 1, early)

            @pl.loop(0, 2)
            def _(side):
                first_pass(lax.rem(z + nz + r - 2 * r * side, nz))

            if 2 < r + 1:
                z_forward(r + 1, late if r + 1 < nz // 2 else early)
        first_pass(z_at(nz // 2))
    with jax.named_scope("lse"):
        tops = peaks[...]
        top = jnp.max(tops, axis=0)
        lses[me] = top + jnp.log(jnp.sum(sums[...] * jnp.exp(tops - top[None]), axis=0))
        for step in range(1, peers):
            send(lses.at[me], lses.at[me], l_send.at[step], l_recv.at[step], peer(step))
        for step in range(1, peers):
            arrived(meta_all.at[from_peer(step)], m_recv.at[step])
        for step in range(1, peers):
            arrived(lses.at[from_peer(step)], l_recv.at[step])
        parts = lses[...]
        top = jnp.max(parts, axis=0)
        total = top + jnp.log(jnp.sum(jnp.exp(parts - top[None]), axis=0))
        scale[...] = jnp.exp(tops - total[None])

    lines = lax.broadcasted_iota(jnp.int32, (size, size), 0)

    def second_pass(chunk):
        first = ((chunk * nx + x) * nc + c) * size

        for k in range(peers):
            weight = meta_all[k, 0:1, :]
            target = meta_all[k, 1:2, :].astype(jnp.int32) - first
            t = probs[chunk * peers + k] * (scale[chunk, k : k + 1, :] * weight)
            t = jnp.where(lines == target, t - weight, t)
            ds[block_rows(chunk), k * size : (k + 1) * size] = t.astype(BF16)

        gi_part[chunk] = jnp.dot(ds[block_rows(chunk), :], users[...], preferred_element_type=F32)

    def z_reduce(r, parts_of=((0, 0), (0, 1), (1, 0), (1, 1))):
        for way, half in parts_of:
            sign = signs[way]
            length = chain_length(nz, way, half)
            rows = pl.ds(half * half_size, half_size)
            dest = z_at(sign * (length - r))
            if 1 <= r <= length:
                land = z_land.at[way, half, r - 1]
                arrived(land, zr_recv.at[way, half, r - 1])
                if r < length:
                    land[...] += gi_part[dest, rows]
            if r < length:
                src = gi_part.at[dest, rows] if r == 0 else z_land.at[way, half, r - 1]
                send(src, z_land.at[way, half, r], zr_send.at[way, half, r],
                     zr_recv.at[way, half, r], {"rows_0": z_at(sign)})

    with jax.named_scope("second"):
        second_pass(z_at(nz // 2))
        z_reduce(0, ((0, 0), (1, 1)))
        second_pass(z_at(nz // 2 - 1))
        z_reduce(0, ((0, 1),))
        second_pass(z_at(1 - nz // 2))
        z_reduce(0, ((1, 0),))
        left = 2 * (nz // 2 - 2) + 1

        @pl.loop(0, left)
        def _(i):
            second_pass(lax.rem(z + nz + ((left - i) // 2) * (1 - 2 * lax.rem(i, 2)), nz))

    def user_pass(k):
        gu_part[k] = jnp.dot(items_turned[...], ds[:, block_rows(k)], preferred_element_type=F32)

    def collected(own, land, n):
        pieces = []
        for half in (0, 1):
            got = own[half * half_size : (half + 1) * half_size]
            for way in (0, 1):
                length = chain_length(n, way, half)
                if length:
                    got = got + land[way, half, length - 1]
            pieces.append(got)
        return jnp.concatenate(pieces, axis=0)


    def x_reduce(r, parts_of):
        for way, half in parts_of:
            sign = signs[way]
            length = chain_length(nx, way, half)
            rows = pl.ds(half * half_size, half_size)
            dest = x_at(sign * (length - r))
            if 1 <= r <= length:
                land = x_land.at[way, half, r - 1]
                arrived(land, xr_recv.at[way, half, r - 1])
                if r < length:
                    land[...] += gu_pair[dest, rows]
            if r < length:
                src = gu_pair.at[dest, rows] if r == 0 else x_land.at[way, half, r - 1]
                send(src, x_land.at[way, half, r], xr_send.at[way, half, r],
                     xr_recv.at[way, half, r], {"rows_1": x_at(sign)})

    with jax.named_scope("zr1"):
        z_reduce(1, early)
    with jax.named_scope("userpass"):
        for step in range(nx):
            k = x_at(step) * nc + 1 - c
            user_pass(k)
            send(gu_part.at[k], gu_pair.at[x_at(step)], d_send.at[step], d_recv.at[step], partner)
        for step in range(nx // 2):
            user_pass(x_at(step) * nc + c)
        z_reduce(1, late)
        for step in range(nx // 2, nx):
            user_pass(x_at(step) * nc + c)
        for step in range(nx):
            arrived(gu_pair.at[x_at(step)], d_recv.at[step])
            gu_pair[x_at(step)] += gu_part[x_at(step) * nc + c]
    with jax.named_scope("reduce"):
        x_reduce(0, early)
        x_reduce(0, late)
        for step in range(1, ny):
            arrived(pairs_all.at[y_at(-step)], i_recv.at[step])
        name_slots()

        @pl.loop(1, plane)
        def _(step):
            where, there = far(step)
            send_plainly(ids_out.at[there], ids_land.at[here], n_send.at[step], n_recv.at[step], where)

        ids_land[here] = ids_out[here]
        along_z = [(r, parts) for r in range(2, nz // 2) for parts in (early, late)]
        along_x = [(r, parts) for r in range(1, nx // 2 + 1) for parts in (early, late)]
        for event in along_z[:2]:
            z_reduce(*event)
        along_z = along_z[2:]
        while along_z or along_x:
            if along_x:
                x_reduce(*along_x.pop(0))
            if along_z:
                z_reduce(*along_z.pop(0))
    with jax.named_scope("towerback"):
        gu = collected(gu_pair[x], x_land, nx).astype(BF16)
        pre = pre_keep[...]
        gate = jax.nn.sigmoid(pre)
        back = jnp.dot(w2_ref[...], gu, preferred_element_type=F32)
        grad_pre = (back * gate * (1.0 + pre * (1.0 - gate))).astype(BF16)
        df_keep[0] = jnp.dot(grad_pre, feat_ref[...], preferred_element_type=F32)
        df_keep[1] = jnp.dot(gu, hid_keep[...], preferred_element_type=F32)

    with jax.named_scope("zrlast"):
        send(df_keep.at[1 - c], df_pair, ac_send, ac_recv, partner)
        z_reduce(nz // 2, early)
        gi = collected(gi_part[z], z_land, nz).astype(BF16)
    with jax.named_scope("shares"):
        for to in range(ny):
            cols = slice(to * share, (to + 1) * share)
            share_out[to] = jnp.concatenate([gi[:half_size, cols], gi[half_size:, cols]], axis=1)
        for step in range(1, ny):
            send(share_out.at[y_at(step)], share_in.at[y], s_send.at[step], s_recv.at[step],
                 {"grp": y_at(step)})
        share_in[y] = share_out[y]
    with jax.named_scope("acy"):
        arrived(df_pair, ac_recv)
        y_part[...] = (df_keep[c] + df_pair[...]).reshape(y_part.shape)
        for step in range(1, ny):
            send(y_part.at[y_at(step)], y_land.at[step - 1], ay_send.at[step], ay_recv.at[step],
                 {"grp": y_at(step)})
    with jax.named_scope("readslots"):
        read_slots()
    with jax.named_scope("sharewait"):
        for step in range(1, ny):
            arrived(share_in.at[y_at(-step)], s_recv.at[step])
    with jax.named_scope("slots"):
        slot_lines = lax.broadcasted_iota(jnp.int32, (plane * cap, size), 0)
        for pair in range(ny // 2):
            sides = []
            for g in (2 * pair, 2 * pair + 1):
                chosen = (slot_lines == slots_keep[g]).astype(BF16)
                packed = share_in[g]
                data = jnp.concatenate([packed[:, :share], packed[:, share:]], axis=0)
                sides.append(jnp.dot(chosen, data, preferred_element_type=F32))
            both = jnp.concatenate(sides, axis=1).astype(BF16)
            slotted[:, pair] = both.reshape(plane, cap, 2 * share)

        turns = {8: (4, 5, 6, 3, 7, 2, 1, 0), 4: (2, 3, 1, 0)}[nz]
        ahead = nz // 2 - 1

        def exchange(dz):
            @pl.loop(0 if dz else 1, peers)
            def _(inner):
                step = dz * peers + inner
                where, there = far(step)
                send_plainly(slotted.at[there], landed.at[here], e_send.at[step], e_recv.at[step],
                             where)

        landed[here] = slotted[here]
        acc[...] = jnp.zeros_like(acc)
    with jax.named_scope("ysum"):
        whole = y_part[y]
        for step in range(1, ny):
            arrived(y_land.at[step - 1], ay_recv.at[step])
            whole = whole + y_land[step - 1]
        p_part[...] = whole.reshape(p_part.shape)

        @pl.loop(1, tiles)
        def _(step):
            where, there = far_tile(step)
            send_plainly(p_part.at[there], p_land.at[step], ap_send.at[step], ap_recv.at[step], where)

        for dz in turns[:ahead]:
            exchange(dz)
        p_land[0] = p_part[tile]
    with jax.named_scope("planesum"):
        long = batch * cap
        lines_of = lax.broadcasted_iota(jnp.int32, (high_span, long), 0)
        for b in range(nz // 2):
            for unit, dz in enumerate(turns[2 * b : 2 * b + 2]):
                for g in range(ny):
                    high = high_all[g, pl.ds(z_at(-dz), 1), :]
                    cols = slice((2 * g + unit) * long, (2 * g + unit + 1) * long)
                    spread_right[b, :, cols] = (lines_of == high).astype(BF16)

        @pl.loop(1, tiles)
        def _(step):
            arrived(p_land.at[step], ap_recv.at[step])
            arrived(p_part.at[0], ap_send.at[step])

        own = tower.at[c, y, tile]
        own[...] = jnp.sum(p_land[...], axis=0)

        @pl.loop(1, tiles)
        def _(step):
            where, _ = far_tile(step)
            send_plainly(own, own, gp_send.at[step], gp_recv.at[step], where)

        for dz in turns[ahead:]:
            exchange(dz)
    def add_rows(b):
        for unit, dz in enumerate(turns[2 * b : 2 * b + 2]):
            @pl.loop(0 if dz else 1, peers)
            def _(inner):
                arrived(landed.at[from_far(dz * peers + inner)], e_recv.at[dz * peers + inner])
                arrived(slotted.at[0], e_send.at[dz * peers + inner])

            source = z_at(-dz)
            for pair in range(ny // 2):
                block = landed[pl.ds(source * batch, batch), pair].reshape(long, 2 * share)
                turned = block.T
                for side in (0, 1):
                    g = 2 * pair + side
                    data = turned[side * share : (side + 1) * share, :]
                    low = low_all[g, pl.ds(source, 1), :]
                    cols = slice((2 * g + unit) * long, (2 * g + unit + 1) * long)
                    for at in range(low_count):
                        spread_left[at * share : (at + 1) * share, cols] = data * (
                            low == at
                        ).astype(BF16)
        acc[...] += contract(spread_left[...], spread_right[b], (1, 1))

    with jax.named_scope("add0"):
        add_rows(0)
    with jax.named_scope("planeback"):
        @pl.loop(1, tiles)
        def _(step):
            arrived(tower.at[c, y, from_far_tile(step)], gp_recv.at[step])
            arrived(p_part.at[0], gp_send.at[step])

        for step in range(1, ny):
            send(tower.at[c, y], tower.at[c, y], gy_send.at[step], gy_recv.at[step],
                 {"grp": y_at(step)})
    with jax.named_scope("add1"):
        for b in range(1, nz // 2 - 1):
            add_rows(b)
    with jax.named_scope("yback"):
        for step in range(1, ny):
            arrived(tower.at[c, y_at(-step)], gy_recv.at[step])
        send(tower.at[c], tower.at[c], gc_send, gc_recv, partner)
    with jax.named_scope("add3"):
        add_rows(nz // 2 - 1)
        for at in range(low_count):
            table_ref[:, at * high_span : (at + 1) * high_span] = acc[at * share : (at + 1) * share, :]
    with jax.named_scope("cback"):
        arrived(tower.at[1 - c], gc_recv)
        width = first_ref.shape[0]
        first_ref[...] = tower[0].reshape(width, width).T
        second_ref[...] = tower[1].reshape(width, width).T
    with jax.named_scope("sent"):
        for copy in pending:
            copy.wait_send()


def block_grads(features, w_first, w_second, items, *columns):
    nz, nx, nc = (lax.axis_size(a) for a in ROWS)
    ny = lax.axis_size("grp")
    size, width = items.shape
    peers = nx * nc
    plane, tiles = nz * peers, nz * nx
    cap = max(2, 4 * size // plane)
    share = width // ny
    vmem, dma = pltpu.VMEM, pltpu.SemaphoreType.DMA
    zh, xh = nz // 2, nx // 2
    lane = ny * cap + 64
    tower = (nc, ny, tiles, width // ny // tiles, width)
    return pl.pallas_call(
        functools.partial(block_kernel, nz, nx, nc, ny),
        out_shape=(
            jax.ShapeDtypeStruct((share, ITEMS_DEV), F32),
            jax.ShapeDtypeStruct((width, width), F32),
            jax.ShapeDtypeStruct((width, width), F32),
        ),
        in_specs=[pl.BlockSpec(memory_space=vmem)] * 8,
        out_specs=[pl.BlockSpec(memory_space=vmem)] * 3,
        scratch_shapes=[
            vmem((peers * size, width), BF16),
            vmem((nz, size, width), BF16),
            vmem((width, nz * size), BF16),
            vmem((peers, 2, size), F32),
            vmem((nz, peers, size), F32),
            vmem((nz, peers, size), F32),
            vmem((peers, peers, size), F32),
            vmem((nz, peers, size), F32),
            vmem((nz * peers, size, size), F32),
            vmem((nz * size, peers * size), BF16),
            vmem((nz, size, width), F32),
            vmem((peers, width, size), F32),
            vmem((nx, width, size), F32),
            vmem((2, 2, zh, size // 2, width), F32),
            vmem((2, 2, xh, width // 2, size), F32),
            vmem((width, size), F32),
            vmem((size, width), BF16),
            dma((2, 2, zh)), dma((2, 2, zh)),
            dma((2, 2, xh)), dma((2, 2, xh)),
            dma((2, 2, xh + 1)), dma((2, 2, xh + 1)),
            dma((peers,)), dma((peers,)),
            dma((peers,)), dma((peers,)),
            dma((2, 2, zh)), dma((2, 2, zh)),
            dma((nx,)), dma((nx,)),
            dma((2, 2, xh)), dma((2, 2, xh)),
            vmem((ny, 2, size), F32),
            vmem((ny, 1, size), jnp.int32),
            vmem((plane, 1, lane), jnp.int32),
            vmem((ny, size // 2, 2 * share), BF16),
            vmem((ny, size // 2, 2 * share), BF16),
            vmem((plane, ny // 2, cap, 2 * share), BF16),
            vmem((2, width, width), F32),
            vmem((width, width), F32),
            vmem((ny, width // ny, width), F32),
            vmem((ny - 1, width // ny, width), F32),
            vmem(tower[2:], F32),
            vmem(tower[2:], F32),
            dma((ny,)), dma((ny,)),
            dma((plane,)), dma((plane,)),
            dma((ny,)), dma((ny,)),
            dma((plane,)), dma((plane,)),
            dma, dma,
            dma((ny,)), dma((ny,)),
            dma((tiles,)), dma((tiles,)),
            dma((tiles,)), dma((tiles,)),
            dma((ny,)), dma((ny,)),
            dma, dma,
            vmem((plane, ny // 2, cap, 2 * share), BF16),
            vmem((plane, 1, lane), jnp.int32),
            vmem(tower, F32),
            vmem((ny, nz, peers * cap), jnp.int32),
            vmem((ny, nz, peers * cap), jnp.int32),
            vmem((ITEMS_DEV // HIGH * share, ny * 2 * peers * cap), BF16),
            vmem((nz // 2, HIGH, ny * 2 * peers * cap), BF16),
            vmem((ITEMS_DEV // HIGH * share, HIGH), F32),
        ],
        compiler_params=pltpu.CompilerParams(
            collective_id=0, has_side_effects=True, vmem_limit_bytes=60 * 2**20
        ),
        cost_estimate=pl.CostEstimate(flops=7 * 10**9, bytes_accessed=2**20, transcendentals=2**22),
        name="block_grads",
    )(features, w_first, w_second, items, *columns)


def finish_kernel(*refs):
    count = (len(refs) - 1) // 2
    copies = [
        pltpu.make_async_copy(refs[i], refs[count + i], refs[-1].at[i]) for i in range(count)
    ]
    for copy in copies:
        copy.start()
    for copy in copies:
        copy.wait()


def finish(*arrays):
    return pl.pallas_call(
        finish_kernel,
        out_shape=tuple(jax.ShapeDtypeStruct(a.shape, a.dtype) for a in arrays),
        in_specs=[pl.BlockSpec(memory_space=pl.ANY)] * len(arrays),
        out_specs=[pl.BlockSpec(memory_space=pltpu.VMEM)] * len(arrays),
        scratch_shapes=[pltpu.SemaphoreType.DMA((len(arrays),))],
        name="finish",
    )(*arrays)


def body(
    user_features, w_first, w_second, item_embed, example_weight, positive, item_owner, item_row
):
    table, first, second = block_grads(
        user_features[0], w_first, w_second, item_embed[0],
        example_weight, positive, item_owner.reshape(positive.shape), item_row,
    )
    table, first, second = finish(table, first, second)
    return (first, second, table.T)


def solution(mesh):
    torus = Mesh(
        mesh.devices.reshape(8, 4, 2, mesh.shape["grp"]), ("rows_0", "rows_1", "rows_2", "grp")
    )
    placed = (
        P("grp", ROWS, None),
        P(),
        P(),
        P("grp", ROWS, None),
        P("grp", ROWS),
        P("grp", ROWS),
        P("grp", ROWS, None),
        P("grp", ROWS),
    )
    return jax.shard_map(
        body, mesh=torus, in_specs=placed, out_specs=(P(), P(), P(ROWS, "grp")), check_vma=False
    )
```
